128 devices in a mesh: rows: 64 (over x_lo, y, z, core), cols: 2 (over x_hi).
Axes of the slice: x: 4 (x_hi: 2, x_lo: 2; x = x_hi * 2 + x_lo), y: 4, z: 4, core: 2. Of those that a mesh axis runs over, the one named last changes fastest.
Arguments:
- design: bfloat16 [131072, 6144], P('rows', 'cols'), may hold values from -0.015625 to 0.015625
- targets: bfloat16 [131072, 128], P('rows'), may hold values from -6 to 6
- col_scale: float32 [6144], P('cols'), may hold values from 0.1 to 1
Outputs:
- solution: float32 [6144, 128], P('cols', 'rows')
- residual: float32 [131072, 128], P('rows')
The draws below stay inside these ranges and needn't reach their ends.
All inputs are finite; a program needn't handle non-finite values.
Results may differ from the reference program's by a relative error of at most 0.0065.
Values may be sent and summed in bfloat16 or wider, within the bound.
A program may use at most 128 MiB of HBM per device.

```python
import math
import jax
import jax.numpy as jnp
from jax import lax

P_SIZE = 6144
FITS = 128
ITERS = 6
M = 131072


def levels(key, shape, cuts, low, high):
    def one(axis_at, shards_of):
        draws = jax.random.uniform(jax.random.fold_in(jax.random.fold_in(key, 6), axis_at), (shards_of,), jnp.float32, low / len(cuts), high / len(cuts))
        return jnp.repeat(jnp.exp(draws), shape[axis_at] // shards_of).reshape((-1,) + (1,) * (len(shape) - axis_at - 1))

    level = one(*cuts[0])
    for cut in cuts[1:]:
        level = level * one(*cut)
    return level


def gaussian(own_key, extent, width, bound, pieces=(), held_as=jnp.bfloat16):
    gain = levels(own_key, extent, pieces, -0.22, 0.18) if pieces else 1.0
    values = jax.random.normal(own_key, extent, jnp.float32) * width * gain
    return jnp.minimum(jnp.maximum(values, -bound), bound).astype(held_as)


def setup_inputs(seed: int = 0) -> dict:
    seeds = jax.random.split(jax.random.key(seed), 4)
    design = gaussian(seeds[0], (M, P_SIZE), M ** -0.5, 0.015625, ((0, 64), (1, 2)))
    targets = gaussian(seeds[1], (M, FITS), 1.0, 6.0, ((0, 64),))
    col_scale = jnp.clip(jnp.exp(math.log(1.0) - 2.3025851 * jax.random.uniform(seeds[2], (P_SIZE,), jnp.float32) ** levels(seeds[2], (P_SIZE,), ((0, 2),), -0.2, 0.2)), 0.1, 1.0)
    return dict(design=design, targets=targets, col_scale=col_scale)


def back_apply(design, scale, vectors):
    product = lax.dot_general(design, vectors, (((0,), (0,)), ((), ())), preferred_element_type=jnp.float32)
    return scale * product


def reference(design, targets, col_scale):
    scale = col_scale[:, None]
    gradient = back_apply(design, scale, targets)
    gamma = jnp.sum(gradient * gradient, axis=0)
    solution = jnp.zeros(gradient.shape, jnp.float32)
    residual = targets.astype(jnp.float32)
    direction = gradient
    for step in range(ITERS):
        scaled_dir = (scale * direction).astype(jnp.bfloat16)
        image = jnp.dot(design, scaled_dir, preferred_element_type=jnp.float32)
        delta = jnp.sum(image * image, axis=0)
        alpha = gamma / delta
        solution = solution + alpha * direction
        residual = residual - alpha * image
        if step + 1 < ITERS:
            gradient = back_apply(design, scale, residual.astype(jnp.bfloat16))
            gamma_new = jnp.sum(gradient * gradient, axis=0)
            direction = gradient + (gamma_new / gamma) * direction
            gamma = gamma_new
    return solution, residual
```

```python
import functools

import jax
import jax.numpy as jnp
from jax import lax
from jax.experimental import pallas as pl
from jax.experimental.pallas import tpu as pltpu
from jax.sharding import PartitionSpec as P

ITERS = 6
NX, NY, NZ, NCORE, NCOL = 2, 4, 4, 2, 2
M_LOC, P_LOC, FITS = 2048, 3072, 128
HALF = FITS // 2
FG = HALF // NZ
LY = P_LOC // NY
CH = 512
NCH = M_LOC // CH
BF, F32 = jnp.bfloat16, jnp.float32
MESH = pl.DeviceIdType.MESH


def wrap_distance(step):
    return min(step, 4 - step)


PLANE = sorted(
    (j for j in range(1, 16)), key=lambda j: -(wrap_distance(j // 4) + wrap_distance(j % 4))
)


def lanes(shape):
    return lax.broadcasted_iota(jnp.int32, shape, len(shape) - 1)


def two_parts(value, first):
    wide = jnp.broadcast_to(value, (value.shape[0], 128))
    high = wide.astype(BF).astype(F32)
    low = (wide - high).astype(BF).astype(F32)
    at = lanes(wide.shape)
    return jnp.where(at == first, high, jnp.where(at == first + 1, low, 0.0))


def kernel(a_hbm, t_ref, s_ref, xo, ro,
           a, q, scal, stile, hacc, hb, hd, hs, dpart, ddp, dlt, rsh, rsd, xs, xr,
           ps, pr, imdp, imdf, res, imt, gv, dv, xv, gam, alf, bet, xpk, fin, fir, fall, fsend,
           a_sem, ex_s, ex_r, d2h_s, d2h_r, d2d_s, d2d_r, rsh_s, rsh_r, rsd_s, rsd_r,
           x_s, x_r, q_s, q_r, sc_s, sc_r, qf_s, qf_r, st_s, st_r, f_s, f_r, g_s, g_r, o_s, o_r):
    r = lax.axis_index("rows")
    col = lax.axis_index("cols")
    core = lax.rem(r, 2)
    chip = r // 2
    z = lax.rem(chip, 4)
    y = lax.rem(chip // 4, 4)
    xl = chip // 16

    def dev(xl_, y_, z_, core_, col_):
        return (((xl_ * 4 + y_) * 4 + z_) * 2 + core_, col_)

    def around(j):
        return lax.rem(y + j // 4, 4), lax.rem(z + j % 4, 4)

    partner = dev(xl, y, z, 1 - core, col)
    across = dev(xl, y, z, core, 1 - col)
    beside = dev(1 - xl, y, z, core, col)

    def remote(src, dst, ss, rs, device):
        return pltpu.make_async_remote_copy(
            src_ref=src, dst_ref=dst, send_sem=ss, recv_sem=rs, device_id=device, device_id_type=MESH)

    for i in range(NCH):
        pltpu.make_async_copy(a_hbm.at[pl.ds(i * CH, CH), :], a.at[pl.ds(i * CH, CH), :], a_sem.at[i]).start()
    barrier = pltpu.get_barrier_semaphore()
    me = r * 2 + col

    def greet(j, carry):
        other = lax.rem(me + j, 128)
        pl.semaphore_signal(barrier, 1, device_id=(other // 2, lax.rem(other, 2)), device_id_type=MESH)
        return carry

    lax.fori_loop(1, 128, greet, 0)
    gv[...] = jnp.zeros(gv.shape, F32)
    dv[...] = jnp.zeros(dv.shape, F32)
    xv[...] = jnp.zeros(xv.shape, F32)
    alf[...] = jnp.zeros(alf.shape, F32)
    bet[...] = jnp.zeros(bet.shape, F32)
    gam[...] = jnp.ones(gam.shape, F32)
    imdf[...] = jnp.zeros(imdf.shape, F32)
    imdp[...] = jnp.zeros(imdp.shape, F32)
    dpart[...] = jnp.zeros(dpart.shape, F32)

    def first_back(i, carry):
        rows = pl.ds(pl.multiple_of(i * CH, CH), CH)
        turned = t_ref[rows, :].astype(F32).T
        res[0, i] = turned[:HALF]
        res[1, i] = turned[HALF:]
        pltpu.make_async_copy(a_hbm.at[rows, :], a.at[rows, :], a_sem.at[i]).wait()
        got = jnp.dot(turned.astype(BF), a[rows, :], preferred_element_type=F32)

        @pl.when(i == 0)
        def _():
            hacc[0] = got[:HALF]
            hacc[1] = got[HALF:]

        @pl.when(i > 0)
        def _():
            hacc[0] += got[:HALF]
            hacc[1] += got[HALF:]

        return carry

    lax.fori_loop(0, NCH, first_back, 0)
    pl.semaphore_wait(barrier, 127)

    def forward(g):
        def chunk(i, carry):
            rows = pl.ds(pl.multiple_of(i * CH, CH), CH)
            part = None
            for b in range(NY):
                term = lax.dot_general(
                    q[g, b], a[rows, b * LY:(b + 1) * LY], (((1,), (1,)), ((), ())),
                    preferred_element_type=F32)
                part = term if part is None else part + term
            part = part + bet[g][:, :1] * imdp[g, i]
            imdp[g, i] = part
            ps[g, i] = part.astype(BF)
            remote(ps.at[g, i], pr.at[g, i], ex_s.at[g, i], ex_r.at[g, i], across).start()
            return carry

        lax.fori_loop(0, NCH, chunk, 0)

    def back(g, t):
        def chunk(i, delta):
            rows = pl.ds(pl.multiple_of(i * CH, CH), CH)
            res[g, i] = res[g, i] - alf[g][:, :1] * imdf[g, i]
            copy = remote(ps.at[g, i], pr.at[g, i], ex_s.at[g, i], ex_r.at[g, i], across)
            copy.wait_recv()
            copy.wait_send()
            image = ps[g, i].astype(F32) + pr[g, i].astype(F32)
            imdf[g, i] = image
            square = image * image
            for b in range(CH // 128):
                delta = delta + square[:, b * 128:(b + 1) * 128]

            @pl.when(t < 2 * ITERS - 2)
            def _():
                got = jnp.dot(image.astype(BF), a[rows, :], preferred_element_type=F32)

                @pl.when(i == 0)
                def _():
                    hacc[g] = got

                @pl.when(i > 0)
                def _():
                    hacc[g] += got

            return delta

        dpart[g] = lax.fori_loop(0, NCH, chunk, jnp.zeros((HALF, 128), F32))

    def to_owner(g):
        @pl.when(core != g)
        def _():
            for b in range(NY):
                hb[b] = hacc[g, :, b * LY:(b + 1) * LY].astype(BF)
            remote(hb, hd, d2h_s, d2h_r, partner).start()
            remote(dpart.at[g], ddp, d2d_s, d2d_r, partner).start()

        @pl.when(core == g)
        def _():
            big = remote(hb, hd, d2h_s, d2h_r, partner)
            small = remote(dpart.at[g], ddp, d2d_s, d2d_r, partner)
            small.wait_recv()
            delta = jnp.sum(dpart[g] + ddp[...], axis=1, keepdims=True)
            dlt[...] = two_parts(delta, 0).astype(BF)
            big.wait_recv()
            for b in range(NY):
                hs[b] = (hacc[g, :, b * LY:(b + 1) * LY] + hd[b].astype(F32)).astype(BF)
            for j in PLANE:
                y_, z_ = around(j)
                to = dev(xl, y_, z_, core, col)
                rows = pl.ds(pl.multiple_of(z_ * FG, FG), FG)
                remote(hs.at[y_, rows, :], rsh.at[j], rsh_s, rsh_r, to).start()
                remote(dlt.at[rows, :], rsd.at[j], rsd_s, rsd_r, to).start()

    my_rows = pl.ds(pl.multiple_of(z * FG, FG), FG)

    def plane_sum(g, it):
        @pl.when(core == g)
        def _():
            p = lax.rem(it, 2)
            total = hs[y, my_rows, :].astype(F32)
            tile = dlt[my_rows, :].astype(F32)
            big = remote(rsh.at[pl.ds(1, 15)], rsh.at[pl.ds(1, 15)], rsh_s, rsh_r, partner)
            small = remote(rsd.at[pl.ds(1, 15)], rsd.at[pl.ds(1, 15)], rsd_s, rsd_r, partner)
            small.wait_recv()
            big.wait_recv()
            for j in range(1, 16):
                total = total + rsh[j].astype(F32)
                tile = tile + rsd[j].astype(F32)
            xs[p, :, :LY] = total
            xs[p, :, LY:] = tile
            remote(xs.at[p], xr.at[p], x_s.at[p], x_r.at[p], beside).start()
            big.wait_send()
            small.wait_send()

    def update(g, it):
        @pl.when(core == g)
        def _():
            p = lax.rem(it, 2)
            scale = s_ref[y]
            gamma = gam[g, my_rows, :][:, :1]
            beta = bet[g, my_rows, :][:, :1]
            direction = gv[...] + beta * dv[...]
            dv[...] = direction
            copy = remote(xs.at[p], xr.at[p], x_s.at[p], x_r.at[p], beside)
            copy.wait()
            both = xs[p] + xr[p]
            delta = jnp.sum(both[:, LY:], axis=1, keepdims=True)
            alpha = jnp.where(it == 0, -1.0, gamma / jnp.where(it == 0, 1.0, delta))
            grad = gv[...] - alpha * (scale * both[:, :LY])
            gv[...] = grad
            q[g, y, my_rows, :] = (scale * grad).astype(BF)
            square = jnp.sum(grad * grad, axis=1, keepdims=True)
            slot = col * 4 + y
            scal[slot, my_rows, :] = (two_parts(square, 0) + two_parts(alpha, 2)).astype(BF)
            for j in PLANE:
                y_, z_ = around(j)
                to = dev(xl, y_, z_, core, col)
                remote(q.at[g, y, my_rows, :], q.at[g, y, my_rows, :], q_s, q_r, to).start()
                far = dev(xl, y_, z_, core, 1 - col)
                remote(scal.at[slot, my_rows, :], scal.at[slot, my_rows, :], sc_s, sc_r, far).start()
                remote(scal.at[slot, my_rows, :], scal.at[slot, my_rows, :], sc_s, sc_r, to).start()
            far = dev(xl, y, z, core, 1 - col)
            remote(scal.at[slot, my_rows, :], scal.at[slot, my_rows, :], sc_s, sc_r, far).start()
            xv[...] = xv[...] + alpha * direction

    def share(g, it):
        @pl.when(core == g)
        def _():
            big = remote(rsh.at[pl.ds(1, 15)], rsh.at[pl.ds(1, 15)], q_s, q_r, partner)
            small = remote(rsd.at[pl.ds(1, 31)], rsd.at[pl.ds(1, 31)], sc_s, sc_r, partner)
            big.wait_recv()
            remote(q.at[g], q.at[g], qf_s, qf_r, partner).start()
            small.wait_recv()
            tile = scal[0].astype(F32)
            for b in range(1, 8):
                tile = tile + scal[b].astype(F32)
            stile[g] = tile
            remote(stile.at[g], stile.at[g], st_s, st_r, partner).start()
            big.wait_send()
            small.wait_send()

        @pl.when(core != g)
        def _():
            remote(hb, hd, d2h_s, d2h_r, partner).wait_send()
            remote(dpart.at[g], ddp, d2d_s, d2d_r, partner).wait_send()
            remote(stile.at[g], stile.at[g], st_s, st_r, partner).wait_recv()

        tile = stile[g]
        at = lanes(tile.shape)
        new = jnp.sum(jnp.where(at < 2, tile, 0.0), axis=1, keepdims=True)
        alpha = jnp.sum(jnp.where(at < 2, 0.0, tile), axis=1, keepdims=True) * 0.125
        old = gam[g][:, :1]
        beta = jnp.where(it == 0, 0.0, new / jnp.where(it == 0, 1.0, old))
        gam[g] = jnp.broadcast_to(new, (HALF, 128))
        alf[g] = jnp.broadcast_to(alpha, (HALF, 128))
        bet[g] = jnp.broadcast_to(beta, (HALF, 128))

        @pl.when(core != g)
        def _():
            remote(q.at[g], q.at[g], qf_s, qf_r, partner).wait_recv()

        @pl.when(core == g)
        def _():
            remote(q.at[g], q.at[g], qf_s, qf_r, partner).wait_send()
            remote(stile.at[g], stile.at[g], st_s, st_r, partner).wait_send()

    to_owner(0)
    to_owner(1)
    plane_sum(0, 0)
    update(0, 0)
    share(0, 0)

    def half_step(t, carry):
        g = lax.rem(t, 2)
        o = 1 - g
        it = (t + 1) // 2
        forward(g)

        @pl.when(t < 2 * ITERS - 1)
        def _():
            plane_sum(o, it)
            update(o, it)

        back(g, t)

        @pl.when(t < 2 * ITERS - 2)
        def _():
            to_owner(g)

        @pl.when(t < 2 * ITERS - 1)
        def _():
            share(o, it)

        return carry

    lax.fori_loop(0, 2 * ITERS, half_step, 0)

    delta = jnp.concatenate(
        [jnp.sum(dpart[g], axis=1, keepdims=True) for g in range(2)], axis=0)
    fin[...] = jnp.broadcast_to(delta, (FITS, 128)).T[:8]
    copy = remote(fin, fir, f_s, f_r, partner)
    copy.start()

    def turn(i, carry):
        rows = pl.ds(pl.multiple_of(i * CH, CH), CH)
        ro[rows, :] = jnp.concatenate([res[0, i], res[1, i]], axis=0).T
        return carry

    lax.fori_loop(0, NCH, turn, 0)
    copy.wait()
    total = fin[...] + fir[...]
    fsend[...] = total
    fall[chip] = total

    def spread(j, carry):
        xl_ = lax.rem(xl + j // 16, 2)
        y_ = lax.rem(y + lax.rem(j // 4, 4), 4)
        z_ = lax.rem(z + lax.rem(j, 4), 4)
        remote(fsend, fall.at[chip], g_s, g_r, dev(xl_, y_, z_, core, col)).start()
        return carry

    lax.fori_loop(1, 32, spread, 0)

    def turn2(i, carry):
        rows = pl.ds(pl.multiple_of(i * CH, CH), CH)
        imt[rows, :] = jnp.concatenate([imdf[0, i], imdf[1, i]], axis=0).T
        return carry

    lax.fori_loop(0, NCH, turn2, 0)
    gamma_lane = jnp.concatenate([gam[0], gam[1]], axis=0).T[:8]
    everyone = remote(fall.at[pl.ds(0, 31)], fall.at[pl.ds(0, 31)], g_s, g_r, partner)
    everyone.wait_recv()
    total = fall[0]
    for b in range(1, 32):
        total = total + fall[b]
    alpha_lane = gamma_lane / total
    alpha_col = jnp.broadcast_to(alpha_lane[:1], (128, 128)).T
    alf[0] = alpha_col[:HALF]
    alf[1] = alpha_col[HALF:]
    alpha = alf[core, my_rows, :][:, :1]
    beta = bet[core, my_rows, :][:, :1]
    solved = xv[...] + alpha * (gv[...] + beta * dv[...])
    for b in range(FG // 2):
        xpk[b] = solved[2 * b:2 * b + 2, :]
    my_lanes = pl.ds(pl.multiple_of(y * LY, LY), LY)
    for b in range(FG // 2):
        mine = (y == z) & (z == b // 2) & (core == b % 2)

        @pl.when((xl == core) & jnp.logical_not(mine))
        def _():
            remote(xpk.at[b], xo.at[:, my_lanes], o_s.at[b], o_r.at[y],
                   dev(core, z, b // 2, b % 2, col)).start()

        @pl.when((xl == core) & mine)
        def _():
            xo[:, my_lanes] = xpk[b]

    def finish(i, carry):
        rows = pl.ds(pl.multiple_of(i * CH, CH), CH)
        ro[rows, :] = ro[rows, :] - alpha_lane[:1] * imt[rows, :]
        return carry

    lax.fori_loop(0, NCH, finish, 0)
    for b in range(NY):
        @pl.when(jnp.logical_not((xl == core) & (y == z) & (y == b)))
        def _():
            remote(xpk.at[0], xo.at[:, b * LY:(b + 1) * LY], o_s.at[0], o_r.at[b], partner).wait_recv()
    for b in range(FG // 2):
        mine = (y == z) & (z == b // 2) & (core == b % 2)

        @pl.when((xl == core) & jnp.logical_not(mine))
        def _():
            remote(xpk.at[b], xo.at[:, my_lanes], o_s.at[b], o_r.at[0], partner).wait_send()
    everyone.wait_send()


def per_device(design, targets, col_scale):
    vm = pltpu.VMEM
    dma = pltpu.SemaphoreType.DMA
    scratch = [
        vm((M_LOC, P_LOC), BF),
        vm((2, NY, HALF, LY), BF),
        vm((8, HALF, 128), BF),
        vm((2, HALF, 128), F32),
        vm((2, HALF, P_LOC), F32),
        vm((NY, HALF, LY), BF),
        vm((NY, HALF, LY), BF),
        vm((NY, HALF, LY), BF),
        vm((2, HALF, 128), F32),
        vm((HALF, 128), F32),
        vm((HALF, 128), BF),
        vm((16, FG, LY), BF),
        vm((32, FG, 128), BF),
        vm((2, FG, LY + 128), F32),
        vm((2, FG, LY + 128), F32),
        vm((2, NCH, HALF, CH), BF),
        vm((2, NCH, HALF, CH), BF),
        vm((2, NCH, HALF, CH), F32),
        vm((2, NCH, HALF, CH), F32),
        vm((2, NCH, HALF, CH), F32),
        vm((M_LOC, FITS), F32),
        vm((FG, LY), F32),
        vm((FG, LY), F32),
        vm((FG, LY), F32),
        vm((2, HALF, 128), F32),
        vm((2, HALF, 128), F32),
        vm((2, HALF, 128), F32),
        vm((FG // 2, 2, LY), F32),
        vm((8, 128), F32),
        vm((8, 128), F32),
        vm((32, 8, 128), F32),
        vm((8, 128), F32),
        dma((NCH,)),
        dma((2, NCH)), dma((2, NCH)),
        dma(()), dma(()), dma(()), dma(()),
        dma(()), dma(()), dma(()), dma(()),
        dma((2,)), dma((2,)),
        dma(()), dma(()), dma(()), dma(()),
        dma(()), dma(()), dma(()), dma(()),
        dma(()), dma(()), dma(()), dma(()),
        dma((FG // 2,)), dma((NY,)),
    ]
    vmem = pl.BlockSpec(memory_space=pltpu.VMEM)
    xo, ro = pl.pallas_call(
        kernel,
        out_shape=(
            jax.ShapeDtypeStruct((2, P_LOC), F32),
            jax.ShapeDtypeStruct((M_LOC, FITS), F32),
        ),
        in_specs=[pl.BlockSpec(memory_space=pl.ANY), vmem, vmem],
        out_specs=(vmem, vmem),
        scratch_shapes=scratch,
        compiler_params=pltpu.CompilerParams(
            collective_id=0, has_side_effects=True, vmem_limit_bytes=48 * 1024 * 1024),
        name="cg_solve",
    )(design, targets, col_scale.reshape(NY, 1, LY))
    return xo.T, ro


def solution(mesh):
    return jax.shard_map(
        per_device, mesh=mesh,
        in_specs=(P("rows", "cols"), P("rows", None), P("cols")),
        out_specs=(P("cols", "rows"), P("rows", None)),
        check_vma=False,
    )
```

```python
import functools

import jax
import jax.numpy as jnp
from jax import lax
from jax.experimental import pallas as pl
from jax.experimental.pallas import tpu as pltpu
from jax.sharding import PartitionSpec as P

ITERS = 6
NX, NY, NZ, NCORE, NCOL = 2, 4, 4, 2, 2
M_LOC, P_LOC, FITS = 2048, 3072, 128
HALF = FITS // 2
FG = HALF // NZ
NBLK = NX * NY
LB = P_LOC // NBLK
CH = 512
NCH = M_LOC // CH
BF, F32 = jnp.bfloat16, jnp.float32
MESH = pl.DeviceIdType.MESH


def wrap_distance(step):
    return min(step, 4 - step)


def far_first(steps, distance):
    return sorted(steps, key=lambda j: -distance(j))


BLOCKS = far_first(range(NBLK), lambda j: j // 4 + wrap_distance(j % 4))
ZS = far_first(range(NZ), wrap_distance)


def rows_and_lanes():
    row = lax.broadcasted_iota(jnp.int32, (FG, 128), 0)
    lane = lax.broadcasted_iota(jnp.int32, (FG, 128), 1)
    return row, lane


def laid_along(column, first):
    row, lane = rows_and_lanes()
    return jnp.sum(jnp.where(lane == row + first, column, 0.0), axis=0, keepdims=True)


def stood_up(line, first):
    row, lane = rows_and_lanes()
    return jnp.sum(jnp.where(lane == row + first, line, 0.0), axis=1, keepdims=True)


def kernel(a_hbm, t_ref, s_ref, xo, ro,
           a, q, scal, stile, hacc, hb, hd, hs, dpart, ddp, dlt, rsh, rsd,
           ps, pr, imdp, imdf, res, imt, gv, dv, xv, gam, alf, bet, xpk, fin, fir, fall, fsend,
           a_sem, ex_s, ex_r, d2h_s, d2h_r, d2d_s, d2d_r, rsh_s, rsh_r, rsd_s, rsd_r,
           q_s, q_r, sc_s, sc_r, qf_s, qf_r, st_s, st_r, f_s, f_r, g_s, g_r, o_s, o_r):
    r = lax.axis_index("rows")
    col = lax.axis_index("cols")
    core = lax.rem(r, 2)
    chip = r // 2
    z = lax.rem(chip, 4)
    y = lax.rem(chip // 4, 4)
    xl = chip // 16

    def dev(xl_, y_, z_, core_, col_):
        return (((xl_ * 4 + y_) * 4 + z_) * 2 + core_, col_)

    def block_at(j):
        return lax.rem(xl + j // 4, 2), lax.rem(y + j % 4, 4)

    def lanes_of(xl_, y_):
        return pl.ds(pl.multiple_of((xl_ * 4 + y_) * LB, LB), LB)

    def rows_of(z_):
        return pl.ds(pl.multiple_of(z_ * FG, FG), FG)

    my_rows = rows_of(z)
    my_lanes = lanes_of(xl, y)
    block = xl * 4 + y
    partner = dev(xl, y, z, 1 - core, col)
    across = dev(xl, y, z, core, 1 - col)

    def remote(src, dst, ss, rs, device):
        return pltpu.make_async_remote_copy(
            src_ref=src, dst_ref=dst, send_sem=ss, recv_sem=rs, device_id=device, device_id_type=MESH)

    for i in range(NCH):
        pltpu.make_async_copy(a_hbm.at[pl.ds(i * CH, CH), :], a.at[pl.ds(i * CH, CH), :], a_sem.at[i]).start()
    barrier = pltpu.get_barrier_semaphore()
    place = ((col * 2 + xl) * 4 + y) * 4 + z

    def greet(j, carry):
        w = lax.rem(place + j, 64)
        other = dev(lax.rem(w // 16, 2), lax.rem(w // 4, 4), lax.rem(w, 4), core, w // 32)
        pl.semaphore_signal(barrier, 1, device_id=other, device_id_type=MESH)
        return carry

    lax.fori_loop(1, 64, greet, 0)
    pl.semaphore_signal(barrier, 1, device_id=partner, device_id_type=MESH)

    def first_back(i, carry):
        rows = pl.ds(pl.multiple_of(i * CH, CH), CH)
        turned = t_ref[rows, :].astype(F32).T
        res[0, i] = turned[:HALF]
        res[1, i] = turned[HALF:]
        pltpu.make_async_copy(a_hbm.at[rows, :], a.at[rows, :], a_sem.at[i]).wait()
        got = jnp.dot(turned.astype(BF), a[rows, :], preferred_element_type=F32)

        @pl.when(i == 0)
        def _():
            hacc[0] = got[:HALF]
            hacc[1] = got[HALF:]

        @pl.when(i > 0)
        def _():
            hacc[0] += got[:HALF]
            hacc[1] += got[HALF:]

        return carry

    lax.fori_loop(0, NCH, first_back, 0)
    gv[...] = jnp.zeros(gv.shape, F32)
    dv[...] = jnp.zeros(dv.shape, F32)
    xv[...] = jnp.zeros(xv.shape, F32)
    alf[...] = jnp.zeros(alf.shape, F32)
    bet[...] = jnp.zeros(bet.shape, F32)
    gam[...] = jnp.ones(gam.shape, F32)
    imdf[...] = jnp.zeros(imdf.shape, F32)
    imdp[...] = jnp.zeros(imdp.shape, F32)
    dpart[...] = jnp.zeros(dpart.shape, F32)
    pl.semaphore_wait(barrier, 64)

    def forward(g):
        def chunk(i, carry):
            rows = pl.ds(pl.multiple_of(i * CH, CH), CH)
            part = lax.dot_general(
                q[g], a[rows, :], (((1,), (1,)), ((), ())), preferred_element_type=F32)
            part = part + bet[g][:, :1] * imdp[g, i]
            imdp[g, i] = part
            ps[g, i] = part.astype(BF)
            remote(ps.at[g, i], pr.at[g, i], ex_s.at[g, i], ex_r.at[g, i], across).start()
            return carry

        lax.fori_loop(0, NCH, chunk, 0)

    def back(g, t):
        def chunk(i, delta):
            rows = pl.ds(pl.multiple_of(i * CH, CH), CH)
            res[g, i] = res[g, i] - alf[g][:, :1] * imdf[g, i]
            copy = remote(ps.at[g, i], pr.at[g, i], ex_s.at[g, i], ex_r.at[g, i], across)
            copy.wait_recv()
            copy.wait_send()
            image = ps[g, i].astype(F32) + pr[g, i].astype(F32)
            imdf[g, i] = image
            square = image * image
            for b in range(CH // 128):
                delta = delta + square[:, b * 128:(b + 1) * 128]

            @pl.when(t < 2 * ITERS - 2)
            def _():
                got = jnp.dot(image.astype(BF), a[rows, :], preferred_element_type=F32)

                @pl.when(i == 0)
                def _():
                    hacc[g] = got

                @pl.when(i > 0)
                def _():
                    hacc[g] += got

            return delta

        dpart[g] = lax.fori_loop(0, NCH, chunk, jnp.zeros((HALF, 128), F32))

    def to_owner(g):
        @pl.when(core != g)
        def _():
            remote(dpart.at[g], ddp, d2d_s, d2d_r, partner).start()
            for j in BLOCKS:
                at = lanes_of(*block_at(j))
                hb[:, at] = hacc[g, :, at].astype(BF)
                remote(hb.at[:, at], hd.at[:, at], d2h_s.at[j], d2h_r.at[j], partner).start()

        @pl.when(core == g)
        def _():
            remote(dpart.at[g], ddp, d2d_s, d2d_r, partner).wait_recv()
            delta = jnp.sum(dpart[g] + ddp[...], axis=1, keepdims=True)
            for b in range(NZ):
                dlt[b] = laid_along(delta[b * FG:(b + 1) * FG], 0)
            for j in BLOCKS:
                xl_, y_ = block_at(j)
                at = lanes_of(xl_, y_)
                remote(hb.at[:, at], hd.at[:, at], d2h_s.at[j], d2h_r.at[j], partner).wait_recv()
                hs[:, at] = (hacc[g, :, at] + hd[:, at].astype(F32)).astype(BF)
                for dz in ZS:
                    if j or dz:
                        z_ = lax.rem(z + dz, 4)
                        to = dev(xl_, y_, z_, core, col)
                        remote(hs.at[rows_of(z_), at], rsh.at[j * 4 + dz], rsh_s, rsh_r, to).start()
                        remote(dlt.at[z_], rsd.at[j * 4 + dz], rsd_s, rsd_r, to).start()

    def update(g, it):
        @pl.when(core == g)
        def _():
            scale = s_ref[block]
            gamma = gam[g, my_rows, :][:, :1]
            beta = bet[g, my_rows, :][:, :1]
            direction = gv[...] + beta * dv[...]
            dv[...] = direction
            big = remote(rsh.at[pl.ds(1, 31)], rsh.at[pl.ds(1, 31)], rsh_s, rsh_r, partner)
            small = remote(rsd.at[pl.ds(1, 31)], rsd.at[pl.ds(1, 31)], rsd_s, rsd_r, partner)
            small.wait_recv()
            line = dlt[z]
            for j in range(1, 32):
                line = line + rsd[j]
            delta = stood_up(line, 0)
            alpha = jnp.where(it == 0, -1.0, gamma / jnp.where(it == 0, 1.0, delta))
            big.wait_recv()
            total = hs[my_rows, my_lanes].astype(F32)
            for j in range(1, 32):
                total = total + rsh[j].astype(F32)
            grad = gv[...] - alpha * (scale * total)
            gv[...] = grad
            q[g, my_rows, my_lanes] = (scale * grad).astype(BF)
            square = jnp.sum(grad * grad, axis=1, keepdims=True)
            slot = (col * NBLK + block) * NZ + z
            scal[slot] = laid_along(square, 0) + laid_along(alpha, FG)
            for j in BLOCKS:
                xl_, y_ = block_at(j)
                back_step = (j // 4) * 4 + (4 - j % 4) % 4
                for dz in ZS:
                    z_ = lax.rem(z + dz, 4)
                    far = dev(xl_, y_, z_, core, 1 - col)
                    remote(scal.at[slot], scal.at[slot], sc_s, sc_r, far).start()
                    if j or dz:
                        to = dev(xl_, y_, z_, core, col)
                        remote(q.at[g, my_rows, my_lanes], q.at[g, my_rows, my_lanes],
                               q_s, q_r.at[back_step], to).start()
                        remote(scal.at[slot], scal.at[slot], sc_s, sc_r, to).start()
            xv[...] = xv[...] + alpha * direction
            big.wait_send()
            small.wait_send()

    def share(g, it):
        @pl.when(core == g)
        def _():
            small = remote(scal.at[pl.ds(0, 63)], scal.at[pl.ds(0, 63)], sc_s, sc_r, partner)
            for j in reversed(BLOCKS):
                count = 64 if j else 48
                got = hd.at[pl.ds(0, count), pl.ds(0, LB)]
                remote(got, got, q_s, q_r.at[j], partner).wait_recv()
                at = lanes_of(*block_at(j))
                remote(q.at[g, :, at], q.at[g, :, at], qf_s.at[j], qf_r.at[j], partner).start()
            small.wait_recv()
            for b in range(NZ):
                line = scal[b]
                for k in range(1, 2 * NBLK):
                    line = line + scal[k * NZ + b]
                gsum = stood_up(line, 0)
                asum = stood_up(line, FG) * (1.0 / (2 * NBLK))
                _, lane = rows_and_lanes()
                stile[g, b * FG:(b + 1) * FG, :] = jnp.where(lane == 0, gsum, asum)
            remote(stile.at[g], stile.at[g], st_s, st_r, partner).start()
            sent = rsh.at[pl.ds(1, 31)]
            remote(sent, sent, q_s, q_r.at[0], partner).wait_send()
            small.wait_send()

        @pl.when(core != g)
        def _():
            for j in BLOCKS:
                at = lanes_of(*block_at(j))
                remote(hb.at[:, at], hd.at[:, at], d2h_s.at[j], d2h_r.at[j], partner).wait_send()
            remote(dpart.at[g], ddp, d2d_s, d2d_r, partner).wait_send()
            remote(stile.at[g], stile.at[g], st_s, st_r, partner).wait_recv()

        tile = stile[g]
        new, alpha = tile[:, :1], tile[:, 1:2]
        old = gam[g][:, :1]
        beta = jnp.where(it == 0, 0.0, new / jnp.where(it == 0, 1.0, old))
        gam[g] = jnp.broadcast_to(new, (HALF, 128))
        alf[g] = jnp.broadcast_to(alpha, (HALF, 128))
        bet[g] = jnp.broadcast_to(beta, (HALF, 128))

        @pl.when(core != g)
        def _():
            for j in BLOCKS:
                at = lanes_of(*block_at(j))
                remote(q.at[g, :, at], q.at[g, :, at], qf_s.at[j], qf_r.at[j], partner).wait_recv()

        @pl.when(core == g)
        def _():
            for j in BLOCKS:
                at = lanes_of(*block_at(j))
                remote(q.at[g, :, at], q.at[g, :, at], qf_s.at[j], qf_r.at[j], partner).wait_send()
            remote(stile.at[g], stile.at[g], st_s, st_r, partner).wait_send()

    to_owner(0)
    to_owner(1)
    update(0, 0)
    share(0, 0)

    def half_step(t, carry):
        g = lax.rem(t, 2)
        o = 1 - g
        it = (t + 1) // 2
        forward(g)

        @pl.when(t < 2 * ITERS - 1)
        def _():
            update(o, it)

        back(g, t)

        @pl.when(t < 2 * ITERS - 2)
        def _():
            to_owner(g)

        @pl.when(t < 2 * ITERS - 1)
        def _():
            share(o, it)

        return carry

    lax.fori_loop(0, 2 * ITERS, half_step, 0)

    delta = jnp.concatenate(
        [jnp.sum(dpart[g], axis=1, keepdims=True) for g in range(2)], axis=0)
    fin[...] = jnp.broadcast_to(delta, (FITS, 128)).T[:8]
    copy = remote(fin, fir, f_s, f_r, partner)
    copy.start()

    def turn(i, carry):
        rows = pl.ds(pl.multiple_of(i * CH, CH), CH)
        ro[rows, :] = jnp.concatenate([res[0, i], res[1, i]], axis=0).T
        return carry

    lax.fori_loop(0, NCH, turn, 0)
    copy.wait()
    total = fin[...] + fir[...]
    fsend[...] = total
    fall[chip] = total

    def spread(j, carry):
        xl_ = lax.rem(xl + j // 16, 2)
        y_ = lax.rem(y + lax.rem(j // 4, 4), 4)
        z_ = lax.rem(z + lax.rem(j, 4), 4)
        remote(fsend, fall.at[chip], g_s, g_r, dev(xl_, y_, z_, core, col)).start()
        return carry

    lax.fori_loop(1, 32, spread, 0)

    def turn2(i, carry):
        rows = pl.ds(pl.multiple_of(i * CH, CH), CH)
        imt[rows, :] = jnp.concatenate([imdf[0, i], imdf[1, i]], axis=0).T
        return carry

    lax.fori_loop(0, NCH, turn2, 0)
    gamma_lane = jnp.concatenate([gam[0], gam[1]], axis=0).T[:8]
    everyone = remote(fall.at[pl.ds(0, 31)], fall.at[pl.ds(0, 31)], g_s, g_r, partner)
    everyone.wait_recv()
    total = fall[0]
    for b in range(1, 32):
        total = total + fall[b]
    alpha_lane = gamma_lane / total
    alpha_col = jnp.broadcast_to(alpha_lane[:1], (128, 128)).T
    alf[0] = alpha_col[:HALF]
    alf[1] = alpha_col[HALF:]
    alpha = alf[core, my_rows, :][:, :1]
    beta = bet[core, my_rows, :][:, :1]
    solved = xv[...] + alpha * (gv[...] + beta * dv[...])
    for b in range(FG // 2):
        xpk[b] = solved[2 * b:2 * b + 2, :]
    for b in range(FG // 2):
        mine = (xl == core) & (y == z) & (z == b // 2) & (core == b % 2)

        @pl.when(jnp.logical_not(mine))
        def _():
            remote(xpk.at[b], xo.at[:, my_lanes], o_s.at[b], o_r.at[block],
                   dev(core, z, b // 2, b % 2, col)).start()

        @pl.when(mine)
        def _():
            xo[:, my_lanes] = xpk[b]

    def finish(i, carry):
        rows = pl.ds(pl.multiple_of(i * CH, CH), CH)
        ro[rows, :] = ro[rows, :] - alpha_lane[:1] * imt[rows, :]
        return carry

    lax.fori_loop(0, NCH, finish, 0)
    for b in range(NBLK):
        @pl.when(jnp.logical_not((xl == core) & (y == z) & (block == b)))
        def _():
            remote(xpk.at[0], xo.at[:, b * LB:(b + 1) * LB], o_s.at[0], o_r.at[b], partner).wait_recv()
    for b in range(FG // 2):
        mine = (xl == core) & (y == z) & (z == b // 2) & (core == b % 2)

        @pl.when(jnp.logical_not(mine))
        def _():
            remote(xpk.at[b], xo.at[:, my_lanes], o_s.at[b], o_r.at[0], partner).wait_send()
    everyone.wait_send()


def per_device(design, targets, col_scale):
    vm = pltpu.VMEM
    dma = pltpu.SemaphoreType.DMA
    scratch = [
        vm((M_LOC, P_LOC), BF),
        vm((2, HALF, P_LOC), BF),
        vm((2 * NBLK * NZ, 1, 128), F32),
        vm((2, HALF, 128), F32),
        vm((2, HALF, P_LOC), F32),
        vm((HALF, P_LOC), BF),
        vm((HALF, P_LOC), BF),
        vm((HALF, P_LOC), BF),
        vm((2, HALF, 128), F32),
        vm((HALF, 128), F32),
        vm((NZ, 1, 128), F32),
        vm((32, FG, LB), BF),
        vm((32, 1, 128), F32),
        vm((2, NCH, HALF, CH), BF),
        vm((2, NCH, HALF, CH), BF),
        vm((2, NCH, HALF, CH), F32),
        vm((2, NCH, HALF, CH), F32),
        vm((2, NCH, HALF, CH), F32),
        vm((M_LOC, FITS), F32),
        vm((FG, LB), F32),
        vm((FG, LB), F32),
        vm((FG, LB), F32),
        vm((2, HALF, 128), F32),
        vm((2, HALF, 128), F32),
        vm((2, HALF, 128), F32),
        vm((FG // 2, 2, LB), F32),
        vm((8, 128), F32),
        vm((8, 128), F32),
        vm((32, 8, 128), F32),
        vm((8, 128), F32),
        dma((NCH,)),
        dma((2, NCH)), dma((2, NCH)),
        dma((NBLK,)), dma((NBLK,)),
        dma(()), dma(()),
        dma(()), dma(()), dma(()), dma(()),
        dma(()), dma((NBLK,)),
        dma(()), dma(()),
        dma((NBLK,)), dma((NBLK,)),
        dma(()), dma(()),
        dma(()), dma(()), dma(()), dma(()),
        dma((FG // 2,)), dma((NBLK,)),
    ]
    vmem = pl.BlockSpec(memory_space=pltpu.VMEM)
    xo, ro = pl.pallas_call(
        kernel,
        out_shape=(
            jax.ShapeDtypeStruct((2, P_LOC), F32),
            jax.ShapeDtypeStruct((M_LOC, FITS), F32),
        ),
        in_specs=[pl.BlockSpec(memory_space=pl.ANY), vmem, vmem],
        out_specs=(vmem, vmem),
        scratch_shapes=scratch,
        compiler_params=pltpu.CompilerParams(
            collective_id=0, has_side_effects=True, vmem_limit_bytes=48 * 1024 * 1024),
        name="cg_solve",
    )(design, targets, col_scale.reshape(NBLK, 1, LB))
    return xo.T, ro


def solution(mesh):
    return jax.shard_map(
        per_device, mesh=mesh,
        in_specs=(P("rows", "cols"), P("rows", None), P("cols")),
        out_specs=(P("cols", "rows"), P("rows", None)),
        check_vma=False,
    )
```

```python
import functools

import jax
import jax.numpy as jnp
from jax import lax
from jax.experimental import pallas as pl
from jax.experimental.pallas import tpu as pltpu
from jax.sharding import PartitionSpec as P

ITERS = 6
NX, NY, NZ, NCORE, NCOL = 2, 4, 4, 2, 2
M_LOC, P_LOC, FITS = 2048, 3072, 128
HALF = FITS // 2
FG = HALF // NZ
NBLK = NX * NY
LB = P_LOC // NBLK
CH = 512
NCH = M_LOC // CH
BF, F32 = jnp.bfloat16, jnp.float32
MESH = pl.DeviceIdType.MESH


def wrap_distance(step):
    return min(step, 4 - step)


def far_first(steps, distance):
    return sorted(steps, key=lambda j: -distance(j))


BLOCKS = far_first(range(NBLK), lambda j: j // 4 + wrap_distance(j % 4))
ZS = far_first(range(NZ), wrap_distance)


def across_chunk(tile):
    return jnp.concatenate([tile] * (CH // 128), axis=1)


def rows_and_lanes():
    row = lax.broadcasted_iota(jnp.int32, (FG, 128), 0)
    lane = lax.broadcasted_iota(jnp.int32, (FG, 128), 1)
    return row, lane


def laid_along(column, first):
    row, lane = rows_and_lanes()
    return jnp.sum(jnp.where(lane == row + first, column, 0.0), axis=0, keepdims=True)


def stood_up(line, first):
    row, lane = rows_and_lanes()
    return jnp.sum(jnp.where(lane == row + first, line, 0.0), axis=1, keepdims=True)


def kernel(a_hbm, t_hbm, s_hbm, xo, ro,
           a, at, t_ref, s_ref, q, scal, stile, hacc, hb, hd, hs, dpart, ddp, dlt, rsh, rsd,
           first, ps, pr, imdp, imdf, res, imt, gv, dv, xv, gam, alf, bet, xpk, fall, fsend, xin,
           a_sem, t_sem, s_sem, ex_s, ex_r, d2h_s, d2h_r, d2d_s, d2d_r, rsh_s, rsh_r, rsd_s, rsd_r,
           q_s, q_r, sc_s, sc_r, qf_s, qf_r, st_s, st_r, g_s, g_r, o_s, o_r):
    r = lax.axis_index("rows")
    col = lax.axis_index("cols")
    core = lax.rem(r, 2)
    chip = r // 2
    z = lax.rem(chip, 4)
    y = lax.rem(chip // 4, 4)
    xl = chip // 16

    def dev(xl_, y_, z_, core_, col_):
        return (((xl_ * 4 + y_) * 4 + z_) * 2 + core_, col_)

    def block_at(j):
        return lax.rem(xl + j // 4, 2), lax.rem(y + j % 4, 4)

    def lanes_of(xl_, y_):
        return pl.ds(pl.multiple_of((xl_ * 4 + y_) * LB, LB), LB)

    def rows_of(z_):
        return pl.ds(pl.multiple_of(z_ * FG, FG), FG)

    my_rows = rows_of(z)
    my_lanes = lanes_of(xl, y)
    block = xl * 4 + y
    partner = dev(xl, y, z, 1 - core, col)
    across = dev(xl, y, z, core, 1 - col)

    def remote(src, dst, ss, rs, device):
        return pltpu.make_async_remote_copy(
            src_ref=src, dst_ref=dst, send_sem=ss, recv_sem=rs, device_id=device, device_id_type=MESH)

    pltpu.make_async_copy(t_hbm, t_ref, t_sem).start()
    pltpu.make_async_copy(s_hbm, s_ref, s_sem).start()
    for i in range(NCH):
        pltpu.make_async_copy(a_hbm.at[pl.ds(i * CH, CH), :], a.at[pl.ds(i * CH, CH), :], a_sem.at[i]).start()
    barrier = pltpu.get_barrier_semaphore()
    place = ((col * 2 + xl) * 4 + y) * 4 + z

    def greet(j, carry):
        w = lax.rem(place + j, 64)
        other = dev(lax.rem(w // 16, 2), lax.rem(w // 4, 4), lax.rem(w, 4), core, w // 32)
        pl.semaphore_signal(barrier, 1, device_id=other, device_id_type=MESH)
        return carry

    lax.fori_loop(1, 64, greet, 0)
    pl.semaphore_signal(barrier, 1, device_id=partner, device_id_type=MESH)

    def first_back(i, carry):
        rows = pl.ds(pl.multiple_of(i * CH, CH), CH)
        turned = t_ref[rows, :].astype(F32).T
        res[0, i] = turned[:HALF]
        res[1, i] = turned[HALF:]
        pltpu.make_async_copy(a_hbm.at[rows, :], a.at[rows, :], a_sem.at[i]).wait()
        got = jnp.dot(turned.astype(BF), a[rows, :], preferred_element_type=F32)

        @pl.when(i == 0)
        def _():
            hacc[0] = got[:HALF]
            hacc[1] = got[HALF:]

        @pl.when(i > 0)
        def _():
            hacc[0] += got[:HALF]
            hacc[1] += got[HALF:]

        return carry

    pltpu.make_async_copy(t_hbm, t_ref, t_sem).wait()
    lax.fori_loop(0, NCH, first_back, 0)
    pltpu.make_async_copy(s_hbm, s_ref, s_sem).wait()
    gv[...] = jnp.zeros(gv.shape, F32)
    dv[...] = jnp.zeros(dv.shape, F32)
    xv[...] = jnp.zeros(xv.shape, F32)
    alf[...] = jnp.zeros(alf.shape, F32)
    bet[...] = jnp.zeros(bet.shape, F32)
    gam[...] = jnp.ones(gam.shape, F32)
    imdf[...] = jnp.zeros(imdf.shape, F32)
    imdp[...] = jnp.zeros(imdp.shape, F32)
    dpart[...] = jnp.zeros(dpart.shape, F32)
    pl.semaphore_wait(barrier, 64)

    def turn_design(k, carry):
        eye = (lax.broadcasted_iota(jnp.int32, (256, 256), 0)
               == lax.broadcasted_iota(jnp.int32, (256, 256), 1)).astype(BF)
        part = pl.ds(pl.multiple_of(k * 256, 256), 256)
        for c in range(NCH):
            at[c, part, :] = lax.dot_general(
                eye, a[c * CH:(c + 1) * CH, part], (((1,), (1,)), ((), ())),
                preferred_element_type=F32).astype(BF)
        return carry

    def forward(g, it):
        first[...] = jnp.dot(q[g], at[0], preferred_element_type=F32)
        share_scalars(g, it)
        beta = across_chunk(bet[g])
        for i in range(NCH):
            part = jnp.dot(q[g], at[i], preferred_element_type=F32) if i else first[...]
            part = part + beta * imdp[g, i]
            imdp[g, i] = part
            ps[g, i] = part.astype(BF)
            remote(ps.at[g, i], pr.at[g, i], ex_s.at[g, i], ex_r.at[g, i], across).start()

    def back(g, t):
        @pl.when(core == g)
        def _():
            sent = rsh.at[pl.ds(1, 31)]
            remote(sent, sent, q_s, q_r.at[0], partner).wait_send()
            sent = scal.at[pl.ds(0, 63)]
            remote(sent, sent, sc_s, sc_r, partner).wait_send()
            for j in BLOCKS:
                part = lanes_of(*block_at(j))
                remote(q.at[g, :, part], q.at[g, :, part], qf_s.at[j], qf_r.at[j], partner).wait_send()
            remote(stile.at[g], stile.at[g], st_s, st_r, partner).wait_send()

        hacc[g] = jnp.zeros((HALF, P_LOC), F32)

        def chunk(i, delta):
            rows = pl.ds(pl.multiple_of(i * CH, CH), CH)
            res[g, i] = res[g, i] - across_chunk(alf[g]) * imdf[g, i]
            copy = remote(ps.at[g, i], pr.at[g, i], ex_s.at[g, i], ex_r.at[g, i], across)
            copy.wait_recv()
            copy.wait_send()
            image = ps[g, i].astype(F32) + pr[g, i].astype(F32)
            imdf[g, i] = image
            square = image * image
            for b in range(CH // 128):
                delta = delta + square[:, b * 128:(b + 1) * 128]

            @pl.when(t < 2 * ITERS - 2)
            def _():
                hacc[g] += jnp.dot(image.astype(BF), a[rows, :], preferred_element_type=F32)

            return delta

        dpart[g] = lax.fori_loop(0, NCH, chunk, jnp.zeros((HALF, 128), F32))

    def to_owner(g):
        @pl.when(core != g)
        def _():
            remote(dpart.at[g], ddp, d2d_s, d2d_r, partner).start()
            for j in BLOCKS:
                part = lanes_of(*block_at(j))
                hb[:, part] = hacc[g, :, part].astype(BF)
                remote(hb.at[:, part], hd.at[:, part], d2h_s.at[j], d2h_r.at[j], partner).start()

        @pl.when(core == g)
        def _():
            remote(dpart.at[g], ddp, d2d_s, d2d_r, partner).wait_recv()
            delta = jnp.sum(dpart[g] + ddp[...], axis=1, keepdims=True)
            for b in range(NZ):
                dlt[b] = laid_along(delta[b * FG:(b + 1) * FG], 0)
            for j in BLOCKS:
                xl_, y_ = block_at(j)
                part = lanes_of(xl_, y_)
                remote(hb.at[:, part], hd.at[:, part], d2h_s.at[j], d2h_r.at[j], partner).wait_recv()
                hs[:, part] = (hacc[g, :, part] + hd[:, part].astype(F32)).astype(BF)
                for dz in ZS:
                    if j or dz:
                        z_ = lax.rem(z + dz, 4)
                        to = dev(xl_, y_, z_, core, col)
                        remote(hs.at[rows_of(z_), part], rsh.at[j * 4 + dz], rsh_s, rsh_r, to).start()
            for j in BLOCKS:
                xl_, y_ = block_at(j)
                for dz in ZS:
                    if j or dz:
                        z_ = lax.rem(z + dz, 4)
                        to = dev(xl_, y_, z_, core, col)
                        remote(dlt.at[z_], rsd.at[j * 4 + dz], rsd_s, rsd_r, to).start()

    def update(g, it):
        @pl.when(core == g)
        def _():
            scale = s_ref[block]
            gamma = gam[g, my_rows, :][:, :1]
            beta = bet[g, my_rows, :][:, :1]
            direction = gv[...] + beta * dv[...]
            dv[...] = direction
            big = remote(rsh.at[pl.ds(1, 31)], rsh.at[pl.ds(1, 31)], rsh_s, rsh_r, partner)
            small = remote(rsd.at[pl.ds(1, 31)], rsd.at[pl.ds(1, 31)], rsd_s, rsd_r, partner)
            small.wait_recv()
            line = dlt[z]
            for j in range(1, 32):
                line = line + rsd[j]
            delta = stood_up(line, 0)
            alpha = jnp.where(it == 0, -1.0, gamma / jnp.where(it == 0, 1.0, delta))
            big.wait_recv()
            total = hs[my_rows, my_lanes].astype(F32)
            for j in range(1, 32):
                total = total + rsh[j].astype(F32)
            grad = gv[...] - alpha * (scale * total)
            gv[...] = grad
            q[g, my_rows, my_lanes] = (scale * grad).astype(BF)
            for j in BLOCKS:
                xl_, y_ = block_at(j)
                back_step = (j // 4) * 4 + (4 - j % 4) % 4
                for dz in ZS:
                    if j or dz:
                        to = dev(xl_, y_, lax.rem(z + dz, 4), core, col)
                        remote(q.at[g, my_rows, my_lanes], q.at[g, my_rows, my_lanes],
                               q_s, q_r.at[back_step], to).start()
            square = jnp.sum(grad * grad, axis=1, keepdims=True)
            slot = (col * NBLK + block) * NZ + z
            scal[slot] = laid_along(square, 0) + laid_along(alpha, FG)
            for j in BLOCKS:
                xl_, y_ = block_at(j)
                for dz in ZS:
                    for c in ((1 - col, col) if j or dz else (1 - col,)):
                        to = dev(xl_, y_, lax.rem(z + dz, 4), core, c)
                        remote(scal.at[slot], scal.at[slot], sc_s, sc_r, to).start()
            xv[...] = xv[...] + alpha * direction
            big.wait_send()
            small.wait_send()

    def share(g):
        @pl.when(core == g)
        def _():
            for j in reversed(BLOCKS):
                got = hd.at[pl.ds(0, 64 if j else 48), pl.ds(0, LB)]
                remote(got, got, q_s, q_r.at[j], partner).wait_recv()
                part = lanes_of(*block_at(j))
                remote(q.at[g, :, part], q.at[g, :, part], qf_s.at[j], qf_r.at[j], partner).start()

        @pl.when(core != g)
        def _():
            remote(dpart.at[g], ddp, d2d_s, d2d_r, partner).wait_send()
            for j in BLOCKS:
                part = lanes_of(*block_at(j))
                remote(hb.at[:, part], hd.at[:, part], d2h_s.at[j], d2h_r.at[j], partner).wait_send()
            for j in BLOCKS:
                part = lanes_of(*block_at(j))
                remote(q.at[g, :, part], q.at[g, :, part], qf_s.at[j], qf_r.at[j], partner).wait_recv()

    def share_scalars(g, it):
        @pl.when(core == g)
        def _():
            remote(scal.at[pl.ds(0, 63)], scal.at[pl.ds(0, 63)], sc_s, sc_r, partner).wait_recv()
            for b in range(NZ):
                line = scal[b]
                for k in range(1, 2 * NBLK):
                    line = line + scal[k * NZ + b]
                gsum = stood_up(line, 0)
                asum = stood_up(line, FG) * (1.0 / (2 * NBLK))
                _, lane = rows_and_lanes()
                stile[g, b * FG:(b + 1) * FG, :] = jnp.where(lane == 0, gsum, asum)
            remote(stile.at[g], stile.at[g], st_s, st_r, partner).start()

        @pl.when(core != g)
        def _():
            remote(stile.at[g], stile.at[g], st_s, st_r, partner).wait_recv()

        tile = stile[g]
        new, alpha = tile[:, :1], tile[:, 1:2]
        old = gam[g][:, :1]
        beta = jnp.where(it == 0, 0.0, new / jnp.where(it == 0, 1.0, old))
        gam[g] = jnp.broadcast_to(new, (HALF, 128))
        alf[g] = jnp.broadcast_to(alpha, (HALF, 128))
        bet[g] = jnp.broadcast_to(beta, (HALF, 128))

    to_owner(0)
    lax.fori_loop(0, P_LOC // 256, turn_design, 0)
    update(0, 0)
    to_owner(1)
    share(0)

    def half_step(t, carry):
        g = lax.rem(t, 2)
        o = 1 - g
        it = (t + 1) // 2
        forward(g, t // 2)

        @pl.when(t < 2 * ITERS - 1)
        def _():
            update(o, it)

        back(g, t)

        @pl.when(t < 2 * ITERS - 2)
        def _():
            to_owner(g)

        @pl.when(t < 2 * ITERS - 1)
        def _():
            share(o)

        return carry

    lax.fori_loop(0, 2 * ITERS, half_step, 0)

    delta = jnp.concatenate(
        [jnp.sum(dpart[g], axis=1, keepdims=True) for g in range(2)], axis=0)
    fsend[...] = jnp.broadcast_to(delta, (FITS, 128)).T[:1]
    fall[r] = fsend[...]

    def spread(j, carry):
        remote(fsend, fall.at[r], g_s, g_r, (lax.rem(r + j, 64), col)).start()
        return carry

    lax.fori_loop(1, 64, spread, 0)
    direction = gv[...] + bet[core, my_rows, :][:, :1] * dv[...]
    for b in range(FG // 2):
        xpk[b, :2] = xv[2 * b:2 * b + 2, :]
        xpk[b, 2:] = direction[2 * b:2 * b + 2, :]
    for b in range(FG // 2):
        mine = (xl == core) & (y == z) & (z == b // 2) & (core == b % 2)

        @pl.when(jnp.logical_not(mine))
        def _():
            remote(xpk.at[b], xin.at[block], o_s.at[b], o_r.at[block],
                   dev(core, z, b // 2, b % 2, col)).start()

        @pl.when(mine)
        def _():
            xin[block] = xpk[b]

    def turn(i, carry):
        rows = pl.ds(pl.multiple_of(i * CH, CH), CH)
        ro[rows, :] = jnp.concatenate([res[0, i], res[1, i]], axis=0).T
        return carry

    lax.fori_loop(0, NCH, turn, 0)
    def turn2(i, carry):
        rows = pl.ds(pl.multiple_of(i * CH, CH), CH)
        imt[rows, :] = jnp.concatenate([imdf[0, i], imdf[1, i]], axis=0).T
        return carry

    lax.fori_loop(0, NCH, turn2, 0)
    gamma_lane = jnp.concatenate([gam[0], gam[1]], axis=0).T[:1]
    everyone = remote(fall.at[pl.ds(0, 63)], fall.at[pl.ds(0, 63)], g_s, g_r, partner)
    everyone.wait_recv()
    total = fall[0]
    for b in range(1, 64):
        total = total + fall[b]
    alpha_lane = gamma_lane / total

    def finish(i, carry):
        rows = pl.ds(pl.multiple_of(i * CH, CH), CH)
        ro[rows, :] = ro[rows, :] - alpha_lane * imt[rows, :]
        return carry

    lax.fori_loop(0, NCH, finish, 0)
    mine = lax.broadcasted_iota(jnp.int32, (2, 128), 1) == (
        2 * r + lax.broadcasted_iota(jnp.int32, (2, 128), 0))
    alpha = jnp.sum(jnp.where(mine, alpha_lane, 0.0), axis=1, keepdims=True)
    for b in range(NBLK):
        @pl.when(jnp.logical_not((xl == core) & (y == z) & (block == b)))
        def _():
            remote(xpk.at[0], xin.at[b], o_s.at[0], o_r.at[b], partner).wait_recv()

        xo[:, b * LB:(b + 1) * LB] = xin[b, :2] + alpha * xin[b, 2:]
    for b in range(FG // 2):
        mine = (xl == core) & (y == z) & (z == b // 2) & (core == b % 2)

        @pl.when(jnp.logical_not(mine))
        def _():
            remote(xpk.at[b], xin.at[0], o_s.at[b], o_r.at[0], partner).wait_send()
    everyone.wait_send()


def per_device(design, targets, col_scale):
    vm = pltpu.VMEM
    dma = pltpu.SemaphoreType.DMA
    scratch = [
        vm((M_LOC, P_LOC), BF),
        vm((NCH, P_LOC, CH), BF),
        vm((M_LOC, FITS), BF),
        vm((NBLK, 1, LB), F32),
        vm((2, HALF, P_LOC), BF),
        vm((2 * NBLK * NZ, 1, 128), F32),
        vm((2, HALF, 128), F32),
        vm((2, HALF, P_LOC), F32),
        vm((HALF, P_LOC), BF),
        vm((HALF, P_LOC), BF),
        vm((HALF, P_LOC), BF),
        vm((2, HALF, 128), F32),
        vm((HALF, 128), F32),
        vm((NZ, 1, 128), F32),
        vm((32, FG, LB), BF),
        vm((32, 1, 128), F32),
        vm((HALF, CH), F32),
        vm((2, NCH, HALF, CH), BF),
        vm((2, NCH, HALF, CH), BF),
        vm((2, NCH, HALF, CH), F32),
        vm((2, NCH, HALF, CH), F32),
        vm((2, NCH, HALF, CH), F32),
        vm((M_LOC, FITS), F32),
        vm((FG, LB), F32),
        vm((FG, LB), F32),
        vm((FG, LB), F32),
        vm((2, HALF, 128), F32),
        vm((2, HALF, 128), F32),
        vm((2, HALF, 128), F32),
        vm((FG // 2, 4, LB), F32),
        vm((64, 1, 128), F32),
        vm((1, 128), F32),
        vm((NBLK, 4, LB), F32),
        dma((NCH,)), dma(()), dma(()),
        dma((2, NCH)), dma((2, NCH)),
        dma((NBLK,)), dma((NBLK,)),
        dma(()), dma(()),
        dma(()), dma(()), dma(()), dma(()),
        dma(()), dma((NBLK,)),
        dma(()), dma(()),
        dma((NBLK,)), dma((NBLK,)),
        dma(()), dma(()),
        dma(()), dma(()),
        dma((FG // 2,)), dma((NBLK,)),
    ]
    vmem = pl.BlockSpec(memory_space=pltpu.VMEM)
    xo, ro = pl.pallas_call(
        kernel,
        out_shape=(
            jax.ShapeDtypeStruct((2, P_LOC), F32),
            jax.ShapeDtypeStruct((M_LOC, FITS), F32),
        ),
        in_specs=[pl.BlockSpec(memory_space=pltpu.HBM)] * 3,
        out_specs=(vmem, vmem),
        scratch_shapes=scratch,
        compiler_params=pltpu.CompilerParams(
            collective_id=0, has_side_effects=True, vmem_limit_bytes=50331648),
        name="cg_solve",
    )(
        design,
        pltpu.with_memory_space_constraint(targets, pltpu.HBM),
        pltpu.with_memory_space_constraint(col_scale.reshape(NBLK, 1, LB), pltpu.HBM),
    )
    return xo.T, ro


def solution(mesh):
    return jax.shard_map(
        per_device, mesh=mesh,
        in_specs=(P("rows", "cols"), P("rows", None), P("cols")),
        out_specs=(P("cols", "rows"), P("rows", None)),
        check_vma=False,
    )
```

```python
import functools

import jax
import jax.numpy as jnp
from jax import lax
from jax.experimental import pallas as pl
from jax.experimental.pallas import tpu as pltpu
from jax.sharding import PartitionSpec as P

ITERS = 6
NX, NY, NZ, NCORE, NCOL = 2, 4, 4, 2, 2
M_LOC, P_LOC, FITS = 2048, 3072, 128
HALF = FITS // 2
FG = HALF // NZ
NBLK = NX * NY
LB = P_LOC // NBLK
CH = 512
NCH = M_LOC // CH
PARTS = (512, 512, 512, 256, 256)
STARTS = tuple(sum(PARTS[:k]) for k in range(len(PARTS)))
AHEAD = 1
LAST = pl.ds(STARTS[-1], PARTS[-1])
BF, F32 = jnp.bfloat16, jnp.float32
MESH = pl.DeviceIdType.MESH


def wrap_distance(step):
    return min(step, 4 - step)


def far_first(steps, distance):
    return sorted(steps, key=lambda j: -distance(j))


CROSSING = far_first(range(4, NBLK), lambda j: wrap_distance(j % 4))
NEAR = far_first(range(4), wrap_distance)
BLOCKS = CROSSING + NEAR
ZS = far_first(range(NZ), wrap_distance)


def widened(tile, size):
    return jnp.concatenate([tile] * (size // 128), axis=1)


def rows_and_lanes():
    row = lax.broadcasted_iota(jnp.int32, (FG, 128), 0)
    lane = lax.broadcasted_iota(jnp.int32, (FG, 128), 1)
    return row, lane


def laid_along(column, first):
    row, lane = rows_and_lanes()
    return jnp.sum(jnp.where(lane == row + first, column, 0.0), axis=0, keepdims=True)


def stood_up(line, first):
    row, lane = rows_and_lanes()
    return jnp.sum(jnp.where(lane == row + first, line, 0.0), axis=1, keepdims=True)


def kernel(a_hbm, t_hbm, s_hbm, xo, ro,
           a, at, t_ref, s_ref, q, scal, stile, hacc, hb, hd, hs, dpart, ddp, dlt, rsh, rsd,
           first, last, ps, pr, imdp, imdf, res, imt, gv, dv, xv, gam, alf, bet, xpk, fall, fsend, xin,
           a_sem, t_sem, s_sem, ex_s, ex_r, d2h_s, d2h_r, d2d_s, d2d_r, rsh_s, rsh_r, rsd_s, rsd_r,
           q_s, q_r, sc_s, sc_r, qf_s, qf_r, st_s, st_r, g_s, g_r, o_s, o_r):
    r = lax.axis_index("rows")
    col = lax.axis_index("cols")
    core = lax.rem(r, 2)
    chip = r // 2
    z = lax.rem(chip, 4)
    y = lax.rem(chip // 4, 4)
    xl = chip // 16

    def dev(xl_, y_, z_, core_, col_):
        return (((xl_ * 4 + y_) * 4 + z_) * 2 + core_, col_)

    def block_at(j):
        return lax.rem(xl + j // 4, 2), lax.rem(y + j % 4, 4)

    def lanes_of(xl_, y_):
        return pl.ds(pl.multiple_of((xl_ * 4 + y_) * LB, LB), LB)

    def rows_of(z_):
        return pl.ds(pl.multiple_of(z_ * FG, FG), FG)

    my_rows = rows_of(z)
    my_lanes = lanes_of(xl, y)
    block = xl * 4 + y
    partner = dev(xl, y, z, 1 - core, col)
    across = dev(xl, y, z, core, 1 - col)

    def remote(src, dst, ss, rs, device):
        return pltpu.make_async_remote_copy(
            src_ref=src, dst_ref=dst, send_sem=ss, recv_sem=rs, device_id=device, device_id_type=MESH)

    pltpu.make_async_copy(t_hbm, t_ref, t_sem).start()
    pltpu.make_async_copy(s_hbm, s_ref, s_sem).start()
    for i in range(NCH):
        pltpu.make_async_copy(a_hbm.at[pl.ds(i * CH, CH), :], a.at[pl.ds(i * CH, CH), :], a_sem.at[i]).start()
    barrier = pltpu.get_barrier_semaphore()
    place = ((col * 2 + xl) * 4 + y) * 4 + z

    def greet(j, carry):
        w = lax.rem(place + j, 64)
        other = dev(lax.rem(w // 16, 2), lax.rem(w // 4, 4), lax.rem(w, 4), core, w // 32)
        pl.semaphore_signal(barrier, 1, device_id=other, device_id_type=MESH)
        return carry

    lax.fori_loop(1, 64, greet, 0)
    pl.semaphore_signal(barrier, 1, device_id=partner, device_id_type=MESH)

    def first_back(i, carry):
        rows = pl.ds(pl.multiple_of(i * CH, CH), CH)
        turned = t_ref[rows, :].astype(F32).T
        res[0, :, rows] = turned[:HALF]
        res[1, :, rows] = turned[HALF:]
        pltpu.make_async_copy(a_hbm.at[rows, :], a.at[rows, :], a_sem.at[i]).wait()
        got = jnp.dot(turned.astype(BF), a[rows, :], preferred_element_type=F32)

        @pl.when(i == 0)
        def _():
            hacc[0] = got[:HALF]
            hacc[1] = got[HALF:]

        @pl.when(i > 0)
        def _():
            hacc[0] += got[:HALF]
            hacc[1] += got[HALF:]

        return carry

    pltpu.make_async_copy(t_hbm, t_ref, t_sem).wait()
    lax.fori_loop(0, NCH, first_back, 0)
    pltpu.make_async_copy(s_hbm, s_ref, s_sem).wait()
    gv[...] = jnp.zeros(gv.shape, F32)
    dv[...] = jnp.zeros(dv.shape, F32)
    xv[...] = jnp.zeros(xv.shape, F32)
    alf[...] = jnp.zeros(alf.shape, F32)
    bet[...] = jnp.zeros(bet.shape, F32)
    gam[...] = jnp.ones(gam.shape, F32)
    imdf[...] = jnp.zeros(imdf.shape, F32)
    imdp[...] = jnp.zeros(imdp.shape, F32)
    dpart[...] = jnp.zeros(dpart.shape, F32)
    pl.semaphore_wait(barrier, 64)

    def turn_design(k, carry):
        eye = (lax.broadcasted_iota(jnp.int32, (256, 256), 0)
               == lax.broadcasted_iota(jnp.int32, (256, 256), 1)).astype(BF)
        part = pl.ds(pl.multiple_of(k * 256, 256), 256)
        for c in range(NCH):
            at[part, c * CH:(c + 1) * CH] = lax.dot_general(
                eye, a[c * CH:(c + 1) * CH, part], (((1,), (1,)), ((), ())),
                preferred_element_type=F32).astype(BF)
        return carry

    def image_copy(g, k):
        part = pl.ds(STARTS[k], PARTS[k])
        return remote(ps.at[g, :, part], pr.at[g, :, part], ex_s.at[g, k], ex_r.at[g, k], across)

    def forward(g, it):
        for c in range(AHEAD):
            first[c] = jnp.dot(q[g], at[:, c * CH:(c + 1) * CH], preferred_element_type=F32)
        share_scalars(g, it)
        beta = widened(bet[g], CH)
        for c in range(NCH):
            part = pl.ds(c * CH, CH)
            value = first[c] if c < AHEAD else jnp.dot(q[g], at[:, part], preferred_element_type=F32)
            value = value + beta * imdp[g, :, part]
            imdp[g, :, part] = value
            ps[g, :, part] = value.astype(BF)
            for k, start in enumerate(STARTS):
                if start // CH == c:
                    image_copy(g, k).start()

    def back(g, t):
        @pl.when(core == g)
        def _():
            sent = rsh.at[pl.ds(1, 31)]
            remote(sent, sent, q_s, q_r.at[0], partner).wait_send()
            sent = scal.at[pl.ds(0, 63)]
            remote(sent, sent, sc_s, sc_r, partner).wait_send()
            for j in BLOCKS:
                part = lanes_of(*block_at(j))
                remote(q.at[g, :, part], q.at[g, :, part], qf_s.at[j], qf_r.at[j], partner).wait_send()
            remote(stile.at[g], stile.at[g], st_s, st_r, partner).wait_send()

        hacc[g] = jnp.zeros((HALF, P_LOC), F32)

        delta = jnp.zeros((HALF, 128), F32)
        for k, (start, size) in enumerate(zip(STARTS, PARTS)):
            part = pl.ds(start, size)
            res[g, :, part] = res[g, :, part] - widened(alf[g], size) * imdf[g, :, part]
            copy = image_copy(g, k)
            copy.wait_recv()
            copy.wait_send()
            image = ps[g, :, part].astype(F32) + pr[g, :, part].astype(F32)
            imdf[g, :, part] = image
            square = image * image
            for b in range(size // 128):
                delta = delta + square[:, b * 128:(b + 1) * 128]
            if k < len(PARTS) - 1:
                @pl.when(t < 2 * ITERS - 2)
                def _():
                    hacc[g] += jnp.dot(image.astype(BF), a[part, :], preferred_element_type=F32)
            else:
                last[...] = image.astype(BF)
        dpart[g] = delta

    def to_owner(g, start=False):
        @pl.when(core != g)
        def _():
            remote(dpart.at[g], ddp, d2d_s, d2d_r, partner).start()
            for steps, half in ((CROSSING, 1 - xl), (NEAR, xl)):
                if not start:
                    part = pl.ds(pl.multiple_of(half * (P_LOC // 2), P_LOC // 2), P_LOC // 2)
                    hacc[g, :, part] += jnp.dot(last[...], a[LAST, part], preferred_element_type=F32)
                for j in steps:
                    part = lanes_of(*block_at(j))
                    hb[:, part] = hacc[g, :, part].astype(BF)
                    remote(hb.at[:, part], hd.at[:, part], d2h_s.at[j], d2h_r.at[j], partner).start()

        @pl.when(core == g)
        def _():
            remote(dpart.at[g], ddp, d2d_s, d2d_r, partner).wait_recv()
            delta = jnp.sum(dpart[g] + ddp[...], axis=1, keepdims=True)
            for b in range(NZ):
                dlt[b] = laid_along(delta[b * FG:(b + 1) * FG], 0)
            for j in BLOCKS:
                xl_, y_ = block_at(j)
                for dz in ZS:
                    if j or dz:
                        z_ = lax.rem(z + dz, 4)
                        to = dev(xl_, y_, z_, core, col)
                        remote(dlt.at[z_], rsd.at[j * 4 + dz], rsd_s, rsd_r, to).start()
            if not start:
                hacc[g] += jnp.dot(last[...], a[LAST, :], preferred_element_type=F32)
            for j in BLOCKS:
                xl_, y_ = block_at(j)
                part = lanes_of(xl_, y_)
                remote(hb.at[:, part], hd.at[:, part], d2h_s.at[j], d2h_r.at[j], partner).wait_recv()
                hs[:, part] = (hacc[g, :, part] + hd[:, part].astype(F32)).astype(BF)
                for dz in ZS:
                    if j or dz:
                        z_ = lax.rem(z + dz, 4)
                        to = dev(xl_, y_, z_, core, col)
                        remote(hs.at[rows_of(z_), part], rsh.at[j * 4 + dz], rsh_s, rsh_r, to).start()

    def update(g, it):
        @pl.when(core == g)
        def _():
            scale = s_ref[block]
            gamma = gam[g, my_rows, :][:, :1]
            beta = bet[g, my_rows, :][:, :1]
            direction = gv[...] + beta * dv[...]
            dv[...] = direction
            big = remote(rsh.at[pl.ds(1, 31)], rsh.at[pl.ds(1, 31)], rsh_s, rsh_r, partner)
            small = remote(rsd.at[pl.ds(1, 31)], rsd.at[pl.ds(1, 31)], rsd_s, rsd_r, partner)
            small.wait_recv()
            line = dlt[z]
            for j in range(1, 32):
                line = line + rsd[j]
            delta = stood_up(line, 0)
            alpha = jnp.where(it == 0, -1.0, gamma / jnp.where(it == 0, 1.0, delta))
            big.wait_recv()
            total = hs[my_rows, my_lanes].astype(F32)
            for j in range(1, 32):
                total = total + rsh[j].astype(F32)
            grad = gv[...] - alpha * (scale * total)
            gv[...] = grad
            q[g, my_rows, my_lanes] = (scale * grad).astype(BF)
            slot = (col * NBLK + block) * NZ + z

            def send_scalars(steps, c):
                for j in steps:
                    for dz in ZS:
                        if j or dz or c is not col:
                            to = dev(*block_at(j), lax.rem(z + dz, 4), core, c)
                            remote(scal.at[slot], scal.at[slot], sc_s, sc_r, to).start()

            def send_q(steps):
                for j in steps:
                    back_step = (j // 4) * 4 + (4 - j % 4) % 4
                    for dz in ZS:
                        if j or dz:
                            to = dev(*block_at(j), lax.rem(z + dz, 4), core, col)
                            remote(q.at[g, my_rows, my_lanes], q.at[g, my_rows, my_lanes],
                                   q_s, q_r.at[back_step], to).start()

            send_q(NEAR)
            square = jnp.sum(grad * grad, axis=1, keepdims=True)
            scal[slot] = laid_along(square, 0) + laid_along(alpha, FG)
            send_scalars(BLOCKS, 1 - col)
            send_scalars(CROSSING, col)
            send_q(CROSSING)
            send_scalars(NEAR, col)
            xv[...] = xv[...] + alpha * direction
            big.wait_send()
            small.wait_send()

    def share(g):
        @pl.when(core == g)
        def _():
            for j in NEAR[::-1] + CROSSING:
                got = hd.at[pl.ds(0, 64 if j else 48), pl.ds(0, LB)]
                remote(got, got, q_s, q_r.at[j], partner).wait_recv()
                part = lanes_of(*block_at(j))
                remote(q.at[g, :, part], q.at[g, :, part], qf_s.at[j], qf_r.at[j], partner).start()

        @pl.when(core != g)
        def _():
            remote(dpart.at[g], ddp, d2d_s, d2d_r, partner).wait_send()
            for j in BLOCKS:
                part = lanes_of(*block_at(j))
                remote(hb.at[:, part], hd.at[:, part], d2h_s.at[j], d2h_r.at[j], partner).wait_send()
            for j in BLOCKS:
                part = lanes_of(*block_at(j))
                remote(q.at[g, :, part], q.at[g, :, part], qf_s.at[j], qf_r.at[j], partner).wait_recv()

    def share_scalars(g, it):
        @pl.when(core == g)
        def _():
            remote(scal.at[pl.ds(0, 63)], scal.at[pl.ds(0, 63)], sc_s, sc_r, partner).wait_recv()
            for b in range(NZ):
                line = scal[b]
                for k in range(1, 2 * NBLK):
                    line = line + scal[k * NZ + b]
                gsum = stood_up(line, 0)
                asum = stood_up(line, FG) * (1.0 / (2 * NBLK))
                _, lane = rows_and_lanes()
                stile[g, b * FG:(b + 1) * FG, :] = jnp.where(lane == 0, gsum, asum)
            remote(stile.at[g], stile.at[g], st_s, st_r, partner).start()

        @pl.when(core != g)
        def _():
            remote(stile.at[g], stile.at[g], st_s, st_r, partner).wait_recv()

        tile = stile[g]
        new, alpha = tile[:, :1], tile[:, 1:2]
        old = gam[g][:, :1]
        beta = jnp.where(it == 0, 0.0, new / jnp.where(it == 0, 1.0, old))
        gam[g] = jnp.broadcast_to(new, (HALF, 128))
        alf[g] = jnp.broadcast_to(alpha, (HALF, 128))
        bet[g] = jnp.broadcast_to(beta, (HALF, 128))

    to_owner(0, True)
    lax.fori_loop(0, P_LOC // 256, turn_design, 0)
    update(0, 0)
    to_owner(1, True)
    share(0)

    def half_step(t, carry):
        g = lax.rem(t, 2)
        o = 1 - g
        it = (t + 1) // 2
        forward(g, t // 2)

        @pl.when(t < 2 * ITERS - 1)
        def _():
            update(o, it)

        back(g, t)

        @pl.when(t < 2 * ITERS - 2)
        def _():
            to_owner(g)

        @pl.when(t < 2 * ITERS - 1)
        def _():
            share(o)

        return carry

    lax.fori_loop(0, 2 * ITERS, half_step, 0)

    delta = jnp.concatenate(
        [jnp.sum(dpart[g], axis=1, keepdims=True) for g in range(2)], axis=0)
    fsend[...] = jnp.broadcast_to(delta, (FITS, 128)).T[:1]
    fall[r] = fsend[...]

    def spread(j, carry):
        remote(fsend, fall.at[r], g_s, g_r, (lax.rem(r + j, 64), col)).start()
        return carry

    lax.fori_loop(1, 64, spread, 0)
    direction = gv[...] + bet[core, my_rows, :][:, :1] * dv[...]
    for b in range(FG // 2):
        xpk[b, :2] = xv[2 * b:2 * b + 2, :]
        xpk[b, 2:] = direction[2 * b:2 * b + 2, :]
    for b in range(FG // 2):
        mine = (xl == core) & (y == z) & (z == b // 2) & (core == b % 2)

        @pl.when(jnp.logical_not(mine))
        def _():
            remote(xpk.at[b], xin.at[block], o_s.at[b], o_r.at[block],
                   dev(core, z, b // 2, b % 2, col)).start()

        @pl.when(mine)
        def _():
            xin[block] = xpk[b]

    def turn(i, carry):
        rows = pl.ds(pl.multiple_of(i * CH, CH), CH)
        ro[rows, :] = jnp.concatenate([res[0, :, rows], res[1, :, rows]], axis=0).T
        return carry

    lax.fori_loop(0, NCH, turn, 0)
    def turn2(i, carry):
        rows = pl.ds(pl.multiple_of(i * CH, CH), CH)
        imt[rows, :] = jnp.concatenate([imdf[0, :, rows], imdf[1, :, rows]], axis=0).T
        return carry

    lax.fori_loop(0, NCH, turn2, 0)
    gamma_lane = jnp.concatenate([gam[0], gam[1]], axis=0).T[:1]
    everyone = remote(fall.at[pl.ds(0, 63)], fall.at[pl.ds(0, 63)], g_s, g_r, partner)
    everyone.wait_recv()
    total = fall[0]
    for b in range(1, 64):
        total = total + fall[b]
    alpha_lane = gamma_lane / total

    def finish(i, carry):
        rows = pl.ds(pl.multiple_of(i * CH, CH), CH)
        ro[rows, :] = ro[rows, :] - alpha_lane * imt[rows, :]
        return carry

    lax.fori_loop(0, NCH, finish, 0)
    mine = lax.broadcasted_iota(jnp.int32, (2, 128), 1) == (
        2 * r + lax.broadcasted_iota(jnp.int32, (2, 128), 0))
    alpha = jnp.sum(jnp.where(mine, alpha_lane, 0.0), axis=1, keepdims=True)
    for b in range(NBLK):
        @pl.when(jnp.logical_not((xl == core) & (y == z) & (block == b)))
        def _():
            remote(xpk.at[0], xin.at[b], o_s.at[0], o_r.at[b], partner).wait_recv()

        xo[:, b * LB:(b + 1) * LB] = xin[b, :2] + alpha * xin[b, 2:]
    for b in range(FG // 2):
        mine = (xl == core) & (y == z) & (z == b // 2) & (core == b % 2)

        @pl.when(jnp.logical_not(mine))
        def _():
            remote(xpk.at[b], xin.at[0], o_s.at[b], o_r.at[0], partner).wait_send()
    everyone.wait_send()


def per_device(design, targets, col_scale):
    vm = pltpu.VMEM
    dma = pltpu.SemaphoreType.DMA
    scratch = [
        vm((M_LOC, P_LOC), BF),
        vm((P_LOC, M_LOC), BF),
        vm((M_LOC, FITS), BF),
        vm((NBLK, 1, LB), F32),
        vm((2, HALF, P_LOC), BF),
        vm((2 * NBLK * NZ, 1, 128), F32),
        vm((2, HALF, 128), F32),
        vm((2, HALF, P_LOC), F32),
        vm((HALF, P_LOC), BF),
        vm((HALF, P_LOC), BF),
        vm((HALF, P_LOC), BF),
        vm((2, HALF, 128), F32),
        vm((HALF, 128), F32),
        vm((NZ, 1, 128), F32),
        vm((32, FG, LB), BF),
        vm((32, 1, 128), F32),
        vm((AHEAD, HALF, CH), F32),
        vm((HALF, PARTS[-1]), BF),
        vm((2, HALF, M_LOC), BF),
        vm((2, HALF, M_LOC), BF),
        vm((2, HALF, M_LOC), F32),
        vm((2, HALF, M_LOC), F32),
        vm((2, HALF, M_LOC), F32),
        vm((M_LOC, FITS), F32),
        vm((FG, LB), F32),
        vm((FG, LB), F32),
        vm((FG, LB), F32),
        vm((2, HALF, 128), F32),
        vm((2, HALF, 128), F32),
        vm((2, HALF, 128), F32),
        vm((FG // 2, 4, LB), F32),
        vm((64, 1, 128), F32),
        vm((1, 128), F32),
        vm((NBLK, 4, LB), F32),
        dma((NCH,)), dma(()), dma(()),
        dma((2, len(PARTS))), dma((2, len(PARTS))),
        dma((NBLK,)), dma((NBLK,)),
        dma(()), dma(()),
        dma(()), dma(()), dma(()), dma(()),
        dma(()), dma((NBLK,)),
        dma(()), dma(()),
        dma((NBLK,)), dma((NBLK,)),
        dma(()), dma(()),
        dma(()), dma(()),
        dma((FG // 2,)), dma((NBLK,)),
    ]
    vmem = pl.BlockSpec(memory_space=pltpu.VMEM)
    xo, ro = pl.pallas_call(
        kernel,
        out_shape=(
            jax.ShapeDtypeStruct((2, P_LOC), F32),
            jax.ShapeDtypeStruct((M_LOC, FITS), F32),
        ),
        in_specs=[pl.BlockSpec(memory_space=pltpu.HBM)] * 3,
        out_specs=(vmem, vmem),
        scratch_shapes=scratch,
        compiler_params=pltpu.CompilerParams(
            collective_id=0, has_side_effects=True, vmem_limit_bytes=50331648),
        name="cg_solve",
    )(
        design,
        pltpu.with_memory_space_constraint(targets, pltpu.HBM),
        pltpu.with_memory_space_constraint(col_scale.reshape(NBLK, 1, LB), pltpu.HBM),
    )
    return xo.T, ro


def solution(mesh):
    return jax.shard_map(
        per_device, mesh=mesh,
        in_specs=(P("rows", "cols"), P("rows", None), P("cols")),
        out_specs=(P("cols", "rows"), P("rows", None)),
        check_vma=False,
    )
```

```python
import functools

import jax
import jax.numpy as jnp
from jax import lax
from jax.experimental import pallas as pl
from jax.experimental.pallas import tpu as pltpu
from jax.sharding import PartitionSpec as P

ITERS = 6
NX, NY, NZ, NCORE, NCOL = 2, 4, 4, 2, 2
M_LOC, P_LOC, FITS = 2048, 3072, 128
HALF = FITS // 2
FG = HALF // NZ
NBLK = NX * NY
LB = P_LOC // NBLK
CH = 512
NCH = M_LOC // CH
PARTS = (512, 512, 512, 256, 256)
STARTS = tuple(sum(PARTS[:k]) for k in range(len(PARTS)))
PROMPT = 3
AHEAD = 1
LAST = pl.ds(STARTS[-1], PARTS[-1])
BF, F32 = jnp.bfloat16, jnp.float32
MESH = pl.DeviceIdType.MESH


def wrap_distance(step):
    return min(step, 4 - step)


def far_first(steps, distance):
    return sorted(steps, key=lambda j: -distance(j))


CROSSING = far_first(range(4, NBLK), lambda j: wrap_distance(j % 4))
NEAR = far_first(range(4), wrap_distance)
BLOCKS = CROSSING + NEAR
ZS = far_first(range(NZ), wrap_distance)


def widened(tile, size):
    return jnp.concatenate([tile] * (size // 128), axis=1)


def rows_and_lanes():
    row = lax.broadcasted_iota(jnp.int32, (FG, 128), 0)
    lane = lax.broadcasted_iota(jnp.int32, (FG, 128), 1)
    return row, lane


def laid_along(column, first):
    row, lane = rows_and_lanes()
    return jnp.sum(jnp.where(lane == row + first, column, 0.0), axis=0, keepdims=True)


def stood_up(line, first):
    row, lane = rows_and_lanes()
    return jnp.sum(jnp.where(lane == row + first, line, 0.0), axis=1, keepdims=True)


def kernel(a_hbm, t_hbm, s_hbm, xo, ro,
           a, at, t_ref, s_ref, q, scal, stile, hacc, hb, hd, hs, dpart, ddp, dlt, rsh, rsd,
           first, last, ps, pr, imdp, imdf, res, imt, gv, dv, xv, gam, alf, bet, xpk, fall, fsend, xin,
           a_sem, t_sem, s_sem, ex_s, ex_r, d2h_s, d2h_r, d2d_s, d2d_r, rsh_s, rsh_r, rsd_s, rsd_r,
           q_s, q_r, sc_s, sc_r, qf_s, qf_r, st_s, st_r, g_s, g_r, o_s, o_r):
    r = lax.axis_index("rows")
    col = lax.axis_index("cols")
    core = lax.rem(r, 2)
    chip = r // 2
    z = lax.rem(chip, 4)
    y = lax.rem(chip // 4, 4)
    xl = chip // 16

    def dev(xl_, y_, z_, core_, col_):
        return (((xl_ * 4 + y_) * 4 + z_) * 2 + core_, col_)

    def block_at(j):
        return lax.rem(xl + j // 4, 2), lax.rem(y + j % 4, 4)

    def lanes_of(xl_, y_):
        return pl.ds(pl.multiple_of((xl_ * 4 + y_) * LB, LB), LB)

    def rows_of(z_):
        return pl.ds(pl.multiple_of(z_ * FG, FG), FG)

    my_rows = rows_of(z)
    my_lanes = lanes_of(xl, y)
    block = xl * 4 + y
    partner = dev(xl, y, z, 1 - core, col)
    across = dev(xl, y, z, core, 1 - col)

    def remote(src, dst, ss, rs, device):
        return pltpu.make_async_remote_copy(
            src_ref=src, dst_ref=dst, send_sem=ss, recv_sem=rs, device_id=device, device_id_type=MESH)

    pltpu.make_async_copy(t_hbm, t_ref, t_sem).start()
    pltpu.make_async_copy(s_hbm, s_ref, s_sem).start()
    for i in range(NCH):
        pltpu.make_async_copy(a_hbm.at[pl.ds(i * CH, CH), :], a.at[pl.ds(i * CH, CH), :], a_sem.at[i]).start()
    barrier = pltpu.get_barrier_semaphore()
    place = ((col * 2 + xl) * 4 + y) * 4 + z

    def greet(j, carry):
        w = lax.rem(place + j, 64)
        other = dev(lax.rem(w // 16, 2), lax.rem(w // 4, 4), lax.rem(w, 4), core, w // 32)
        pl.semaphore_signal(barrier, 1, device_id=other, device_id_type=MESH)
        return carry

    lax.fori_loop(1, 64, greet, 0)
    pl.semaphore_signal(barrier, 1, device_id=partner, device_id_type=MESH)

    def first_back(i, carry):
        rows = pl.ds(pl.multiple_of(i * CH, CH), CH)
        turned = t_ref[rows, :].astype(F32).T
        res[0, :, rows] = turned[:HALF]
        res[1, :, rows] = turned[HALF:]
        pltpu.make_async_copy(a_hbm.at[rows, :], a.at[rows, :], a_sem.at[i]).wait()
        got = jnp.dot(turned.astype(BF), a[rows, :], preferred_element_type=F32)

        @pl.when(i == 0)
        def _():
            hacc[0] = got[:HALF]
            hacc[1] = got[HALF:]

        @pl.when(i > 0)
        def _():
            hacc[0] += got[:HALF]
            hacc[1] += got[HALF:]

        return carry

    pltpu.make_async_copy(t_hbm, t_ref, t_sem).wait()
    lax.fori_loop(0, NCH, first_back, 0)
    pltpu.make_async_copy(s_hbm, s_ref, s_sem).wait()
    gv[...] = jnp.zeros(gv.shape, F32)
    dv[...] = jnp.zeros(dv.shape, F32)
    xv[...] = jnp.zeros(xv.shape, F32)
    alf[...] = jnp.zeros(alf.shape, F32)
    bet[...] = jnp.zeros(bet.shape, F32)
    gam[...] = jnp.ones(gam.shape, F32)
    imdf[...] = jnp.zeros(imdf.shape, F32)
    imdp[...] = jnp.zeros(imdp.shape, F32)
    dpart[...] = jnp.zeros(dpart.shape, F32)
    pl.semaphore_wait(barrier, 64)

    def turn_design(k, carry):
        eye = (lax.broadcasted_iota(jnp.int32, (256, 256), 0)
               == lax.broadcasted_iota(jnp.int32, (256, 256), 1)).astype(BF)
        part = pl.ds(pl.multiple_of(k * 256, 256), 256)
        for c in range(NCH):
            at[part, c * CH:(c + 1) * CH] = lax.dot_general(
                eye, a[c * CH:(c + 1) * CH, part], (((1,), (1,)), ((), ())),
                preferred_element_type=F32).astype(BF)
        return carry

    def image_copy(g, k):
        part = pl.ds(STARTS[k], PARTS[k])
        return remote(ps.at[g, :, part], pr.at[g, :, part], ex_s.at[g, k], ex_r.at[g, k], across)

    def forward(g, it):
        for c in range(AHEAD):
            first[c] = jnp.dot(q[g], at[:, c * CH:(c + 1) * CH], preferred_element_type=F32)
        share_scalars(g, it)
        beta = widened(bet[g], CH)
        for c in range(NCH):
            part = pl.ds(c * CH, CH)
            value = first[c] if c < AHEAD else jnp.dot(q[g], at[:, part], preferred_element_type=F32)
            value = value + beta * imdp[g, :, part]
            imdp[g, :, part] = value
            ps[g, :, part] = value.astype(BF)
            for k, start in enumerate(STARTS):
                if start // CH != c:
                    continue
                if k < PROMPT:
                    image_copy(g, k).start()
                else:
                    @pl.when((core != g) | (it == ITERS - 1))
                    def _():
                        image_copy(g, k).start()

    def before_back(g):
        @pl.when(core == g)
        def _():
            sent = rsh.at[pl.ds(1, 31)]
            remote(sent, sent, q_s, q_r.at[0], partner).wait_send()
            sent = scal.at[pl.ds(0, 63)]
            remote(sent, sent, sc_s, sc_r, partner).wait_send()
            for j in BLOCKS:
                part = lanes_of(*block_at(j))
                remote(q.at[g, :, part], q.at[g, :, part], qf_s.at[j], qf_r.at[j], partner).wait_send()
            remote(stile.at[g], stile.at[g], st_s, st_r, partner).wait_send()

        hacc[g] = jnp.zeros((HALF, P_LOC), F32)
        res[g] = res[g] - widened(alf[g], M_LOC) * imdf[g]

    def back(g, t):
        delta = jnp.zeros((HALF, 128), F32)
        for k, (start, size) in enumerate(zip(STARTS, PARTS)):
            part = pl.ds(start, size)
            copy = image_copy(g, k)
            copy.wait_recv()
            if k == 0:
                @pl.when((core == g) & (t < 2 * ITERS - 2))
                def _():
                    for late in range(PROMPT, len(PARTS)):
                        image_copy(g, late).start()
            copy.wait_send()
            image = ps[g, :, part].astype(F32) + pr[g, :, part].astype(F32)
            imdf[g, :, part] = image
            square = image * image
            for b in range(size // 128):
                delta = delta + square[:, b * 128:(b + 1) * 128]
            if k < len(PARTS) - 1:
                @pl.when(t < 2 * ITERS - 2)
                def _():
                    hacc[g] += jnp.dot(image.astype(BF), a[part, :], preferred_element_type=F32)
            else:
                last[...] = image.astype(BF)
        dpart[g] = delta

    def to_owner(g, start=False):
        @pl.when(core != g)
        def _():
            remote(dpart.at[g], ddp, d2d_s, d2d_r, partner).start()
            for steps, half in ((CROSSING, 1 - xl), (NEAR, xl)):
                if not start:
                    part = pl.ds(pl.multiple_of(half * (P_LOC // 2), P_LOC // 2), P_LOC // 2)
                    hacc[g, :, part] += jnp.dot(last[...], a[LAST, part], preferred_element_type=F32)
                for j in steps:
                    part = lanes_of(*block_at(j))
                    hb[:, part] = hacc[g, :, part].astype(BF)
                    remote(hb.at[:, part], hd.at[:, part], d2h_s.at[j], d2h_r.at[j], partner).start()

        @pl.when(core == g)
        def _():
            remote(dpart.at[g], ddp, d2d_s, d2d_r, partner).wait_recv()
            delta = jnp.sum(dpart[g] + ddp[...], axis=1, keepdims=True)
            for b in range(NZ):
                dlt[b] = laid_along(delta[b * FG:(b + 1) * FG], 0)
            for j in BLOCKS:
                xl_, y_ = block_at(j)
                for dz in ZS:
                    if j or dz:
                        z_ = lax.rem(z + dz, 4)
                        to = dev(xl_, y_, z_, core, col)
                        remote(dlt.at[z_], rsd.at[j * 4 + dz], rsd_s, rsd_r, to).start()
            if not start:
                hacc[g] += jnp.dot(last[...], a[LAST, :], preferred_element_type=F32)
            for j in BLOCKS:
                xl_, y_ = block_at(j)
                part = lanes_of(xl_, y_)
                remote(hb.at[:, part], hd.at[:, part], d2h_s.at[j], d2h_r.at[j], partner).wait_recv()
                hs[:, part] = (hacc[g, :, part] + hd[:, part].astype(F32)).astype(BF)
                for dz in ZS:
                    if j or dz:
                        z_ = lax.rem(z + dz, 4)
                        to = dev(xl_, y_, z_, core, col)
                        remote(hs.at[rows_of(z_), part], rsh.at[j * 4 + dz], rsh_s, rsh_r, to).start()

    def update(g, it):
        @pl.when(core == g)
        def _():
            scale = s_ref[block]
            gamma = gam[g, my_rows, :][:, :1]
            beta = bet[g, my_rows, :][:, :1]
            direction = gv[...] + beta * dv[...]
            dv[...] = direction
            big = remote(rsh.at[pl.ds(1, 31)], rsh.at[pl.ds(1, 31)], rsh_s, rsh_r, partner)
            small = remote(rsd.at[pl.ds(1, 31)], rsd.at[pl.ds(1, 31)], rsd_s, rsd_r, partner)
            small.wait_recv()
            line = dlt[z]
            for j in range(1, 32):
                line = line + rsd[j]
            delta = stood_up(line, 0)
            alpha = jnp.where(it == 0, -1.0, gamma / jnp.where(it == 0, 1.0, delta))
            big.wait_recv()
            total = hs[my_rows, my_lanes].astype(F32)
            for j in range(1, 32):
                total = total + rsh[j].astype(F32)
            grad = gv[...] - alpha * (scale * total)
            gv[...] = grad
            q[g, my_rows, my_lanes] = (scale * grad).astype(BF)
            slot = (col * NBLK + block) * NZ + z

            def send_scalars(steps, c):
                for j in steps:
                    for dz in ZS:
                        if j or dz or c is not col:
                            to = dev(*block_at(j), lax.rem(z + dz, 4), core, c)
                            remote(scal.at[slot], scal.at[slot], sc_s, sc_r, to).start()

            def send_q(steps):
                for j in steps:
                    back_step = (j // 4) * 4 + (4 - j % 4) % 4
                    for dz in ZS:
                        if j or dz:
                            to = dev(*block_at(j), lax.rem(z + dz, 4), core, col)
                            remote(q.at[g, my_rows, my_lanes], q.at[g, my_rows, my_lanes],
                                   q_s, q_r.at[back_step], to).start()

            send_q(NEAR)
            square = jnp.sum(grad * grad, axis=1, keepdims=True)
            scal[slot] = laid_along(square, 0) + laid_along(alpha, FG)
            send_scalars(BLOCKS, 1 - col)
            send_scalars(CROSSING, col)
            send_q(CROSSING)
            send_scalars(NEAR, col)
            xv[...] = xv[...] + alpha * direction
            big.wait_send()
            small.wait_send()

    def share(g):
        @pl.when(core == g)
        def _():
            for j in NEAR[::-1] + CROSSING:
                got = hd.at[pl.ds(0, 64 if j else 48), pl.ds(0, LB)]
                remote(got, got, q_s, q_r.at[j], partner).wait_recv()
                part = lanes_of(*block_at(j))
                remote(q.at[g, :, part], q.at[g, :, part], qf_s.at[j], qf_r.at[j], partner).start()

        @pl.when(core != g)
        def _():
            remote(dpart.at[g], ddp, d2d_s, d2d_r, partner).wait_send()
            for j in BLOCKS:
                part = lanes_of(*block_at(j))
                remote(hb.at[:, part], hd.at[:, part], d2h_s.at[j], d2h_r.at[j], partner).wait_send()
            for j in BLOCKS:
                part = lanes_of(*block_at(j))
                remote(q.at[g, :, part], q.at[g, :, part], qf_s.at[j], qf_r.at[j], partner).wait_recv()

    def share_scalars(g, it):
        @pl.when(core == g)
        def _():
            remote(scal.at[pl.ds(0, 63)], scal.at[pl.ds(0, 63)], sc_s, sc_r, partner).wait_recv()
            for b in range(NZ):
                line = scal[b]
                for k in range(1, 2 * NBLK):
                    line = line + scal[k * NZ + b]
                gsum = stood_up(line, 0)
                asum = stood_up(line, FG) * (1.0 / (2 * NBLK))
                _, lane = rows_and_lanes()
                stile[g, b * FG:(b + 1) * FG, :] = jnp.where(lane == 0, gsum, asum)
            remote(stile.at[g], stile.at[g], st_s, st_r, partner).start()

        @pl.when(core != g)
        def _():
            remote(stile.at[g], stile.at[g], st_s, st_r, partner).wait_recv()

        tile = stile[g]
        new, alpha = tile[:, :1], tile[:, 1:2]
        old = gam[g][:, :1]
        beta = jnp.where(it == 0, 0.0, new / jnp.where(it == 0, 1.0, old))
        gam[g] = jnp.broadcast_to(new, (HALF, 128))
        alf[g] = jnp.broadcast_to(alpha, (HALF, 128))
        bet[g] = jnp.broadcast_to(beta, (HALF, 128))

    to_owner(0, True)
    lax.fori_loop(0, P_LOC // 256, turn_design, 0)
    update(0, 0)
    to_owner(1, True)
    share(0)

    def half_step(t, carry):
        g = lax.rem(t, 2)
        o = 1 - g
        it = (t + 1) // 2
        forward(g, t // 2)

        @pl.when(g == 1)
        def _():
            before_back(g)

        @pl.when(t < 2 * ITERS - 1)
        def _():
            update(o, it)

        @pl.when(g == 0)
        def _():
            before_back(g)

        back(g, t)

        @pl.when(t < 2 * ITERS - 2)
        def _():
            to_owner(g)

        @pl.when(t < 2 * ITERS - 1)
        def _():
            share(o)

        return carry

    lax.fori_loop(0, 2 * ITERS, half_step, 0)

    delta = jnp.concatenate(
        [jnp.sum(dpart[g], axis=1, keepdims=True) for g in range(2)], axis=0)
    fsend[...] = jnp.broadcast_to(delta, (FITS, 128)).T[:1]
    fall[r] = fsend[...]

    for j in BLOCKS:
        for dz in ZS:
            for c in (1 - core, core):
                if j or dz or c is not core:
                    to = dev(*block_at(j), lax.rem(z + dz, 4), c, col)
                    remote(fsend, fall.at[r], g_s, g_r, to).start()
    direction = gv[...] + bet[core, my_rows, :][:, :1] * dv[...]
    for b in range(FG // 2):
        xpk[b, :2] = xv[2 * b:2 * b + 2, :]
        xpk[b, 2:] = direction[2 * b:2 * b + 2, :]
    for b in range(FG // 2):
        mine = (xl == core) & (y == z) & (z == b // 2) & (core == b % 2)

        @pl.when(jnp.logical_not(mine))
        def _():
            remote(xpk.at[b], xin.at[block], o_s.at[b], o_r.at[block],
                   dev(core, z, b // 2, b % 2, col)).start()

        @pl.when(mine)
        def _():
            xin[block] = xpk[b]

    def turn(i, carry):
        rows = pl.ds(pl.multiple_of(i * CH, CH), CH)
        ro[rows, :] = jnp.concatenate([res[0, :, rows], res[1, :, rows]], axis=0).T
        return carry

    lax.fori_loop(0, NCH, turn, 0)
    def turn2(i, carry):
        rows = pl.ds(pl.multiple_of(i * CH, CH), CH)
        imt[rows, :] = jnp.concatenate([imdf[0, :, rows], imdf[1, :, rows]], axis=0).T
        return carry

    lax.fori_loop(0, NCH, turn2, 0)
    gamma_lane = jnp.concatenate([gam[0], gam[1]], axis=0).T[:1]
    everyone = remote(fall.at[pl.ds(0, 63)], fall.at[pl.ds(0, 63)], g_s, g_r, partner)
    everyone.wait_recv()
    total = fall[0]
    for b in range(1, 64):
        total = total + fall[b]
    alpha_lane = gamma_lane / total

    def finish(i, carry):
        rows = pl.ds(pl.multiple_of(i * CH, CH), CH)
        ro[rows, :] = ro[rows, :] - alpha_lane * imt[rows, :]
        return carry

    lax.fori_loop(0, NCH, finish, 0)
    mine = lax.broadcasted_iota(jnp.int32, (2, 128), 1) == (
        2 * r + lax.broadcasted_iota(jnp.int32, (2, 128), 0))
    alpha = jnp.sum(jnp.where(mine, alpha_lane, 0.0), axis=1, keepdims=True)
    for b in range(NBLK):
        @pl.when(jnp.logical_not((xl == core) & (y == z) & (block == b)))
        def _():
            remote(xpk.at[0], xin.at[b], o_s.at[0], o_r.at[b], partner).wait_recv()

        xo[:, b * LB:(b + 1) * LB] = xin[b, :2] + alpha * xin[b, 2:]
    for b in range(FG // 2):
        mine = (xl == core) & (y == z) & (z == b // 2) & (core == b % 2)

        @pl.when(jnp.logical_not(mine))
        def _():
            remote(xpk.at[b], xin.at[0], o_s.at[b], o_r.at[0], partner).wait_send()
    everyone.wait_send()


def per_device(design, targets, col_scale):
    vm = pltpu.VMEM
    dma = pltpu.SemaphoreType.DMA
    scratch = [
        vm((M_LOC, P_LOC), BF),
        vm((P_LOC, M_LOC), BF),
        vm((M_LOC, FITS), BF),
        vm((NBLK, 1, LB), F32),
        vm((2, HALF, P_LOC), BF),
        vm((2 * NBLK * NZ, 1, 128), F32),
        vm((2, HALF, 128), F32),
        vm((2, HALF, P_LOC), F32),
        vm((HALF, P_LOC), BF),
        vm((HALF, P_LOC), BF),
        vm((HALF, P_LOC), BF),
        vm((2, HALF, 128), F32),
        vm((HALF, 128), F32),
        vm((NZ, 1, 128), F32),
        vm((32, FG, LB), BF),
        vm((32, 1, 128), F32),
        vm((AHEAD, HALF, CH), F32),
        vm((HALF, PARTS[-1]), BF),
        vm((2, HALF, M_LOC), BF),
        vm((2, HALF, M_LOC), BF),
        vm((2, HALF, M_LOC), F32),
        vm((2, HALF, M_LOC), F32),
        vm((2, HALF, M_LOC), F32),
        vm((M_LOC, FITS), F32),
        vm((FG, LB), F32),
        vm((FG, LB), F32),
        vm((FG, LB), F32),
        vm((2, HALF, 128), F32),
        vm((2, HALF, 128), F32),
        vm((2, HALF, 128), F32),
        vm((FG // 2, 4, LB), F32),
        vm((64, 1, 128), F32),
        vm((1, 128), F32),
        vm((NBLK, 4, LB), F32),
        dma((NCH,)), dma(()), dma(()),
        dma((2, len(PARTS))), dma((2, len(PARTS))),
        dma((NBLK,)), dma((NBLK,)),
        dma(()), dma(()),
        dma(()), dma(()), dma(()), dma(()),
        dma(()), dma((NBLK,)),
        dma(()), dma(()),
        dma((NBLK,)), dma((NBLK,)),
        dma(()), dma(()),
        dma(()), dma(()),
        dma((FG // 2,)), dma((NBLK,)),
    ]
    vmem = pl.BlockSpec(memory_space=pltpu.VMEM)
    xo, ro = pl.pallas_call(
        kernel,
        out_shape=(
            jax.ShapeDtypeStruct((2, P_LOC), F32),
            jax.ShapeDtypeStruct((M_LOC, FITS), F32),
        ),
        in_specs=[pl.BlockSpec(memory_space=pltpu.HBM)] * 3,
        out_specs=(vmem, vmem),
        scratch_shapes=scratch,
        compiler_params=pltpu.CompilerParams(
            collective_id=0, has_side_effects=True, vmem_limit_bytes=50331648),
        name="cg_solve",
    )(
        design,
        pltpu.with_memory_space_constraint(targets, pltpu.HBM),
        pltpu.with_memory_space_constraint(col_scale.reshape(NBLK, 1, LB), pltpu.HBM),
    )
    return xo.T, ro


def solution(mesh):
    return jax.shard_map(
        per_device, mesh=mesh,
        in_specs=(P("rows", "cols"), P("rows", None), P("cols")),
        out_specs=(P("cols", "rows"), P("rows", None)),
        check_vma=False,
    )
```
